256 devices in a mesh: wave: 32 (over z, y), lev: 8 (over x, core).
Axes of the slice: x: 4, y: 4, z: 8, core: 2. Of those that a mesh axis runs over, the one named last changes fastest.
Arguments:
- spectral: bfloat16 [128, 6, 128, 1280], P('wave', None, 'lev'), may hold values from -0.01171875 to 0.01171875
- legendre: bfloat16 [128, 640, 1280], P('wave'), may hold values from -4 to 4
- wave_ids: int32 [128], replicated, may hold values from 0 to 1279, as said below
- trunc_lengths: int32 [128], replicated, may hold values from 1 to 1280, as said below
- cycle_points: int32 [1280], replicated, may hold values from 20 to 2560, as said below
- grid_coef: float32 [1280, 2560], P('wave'), may hold values from -6 to 6
- cycle_weights: float32 [640], replicated, may hold values from 0.1 to 2
- modes_in: bfloat16 [128, 128], replicated, may hold values from -0.5 to 0.5
- modes_out: bfloat16 [128, 128], replicated, may hold values from -0.5 to 0.5
- depths: float32 [128], replicated, may hold values from 0.05 to 20
Outputs:
- update: bfloat16 [128, 6, 128, 1280], P('wave', None, 'lev')
The draws below stay inside these ranges and needn't reach their ends.
Inputs may be any that keep to these rules, and one draw needn't show every extreme that they name: `wave_ids`: distinct zonal wavenumbers; one slot holds wavenumber 0. `trunc_lengths`: the length of slot m is at most 1280 minus wave_ids[m] and at least half of that; the slot of wavenumber 0 has length 1280. `cycle_points`: multiples of 4; cycle j and cycle 1280 - 1-j have the same count; cycles near the equator have 2560.
All inputs are finite; a program needn't handle non-finite values.
Results may differ from the reference program's by a relative error of at most 0.011.
Values may be sent and summed in bfloat16 or wider, within the bound.
A program may use at most 128 MiB of HBM per device.

```python
import math
import jax
import jax.numpy as jnp
from jax import lax

NT = 1280
NLAT = 1280
NHALF = 640
LONMAX = 2560
FIELDS = 3
M_WIN = 128
LEVELS = 128


def wave_table(key):
    base_key = jax.random.fold_in(key, 11)
    others = jax.random.permutation(jax.random.fold_in(base_key, 1), NT - 1)[:M_WIN - 1] + 1
    chosen = jnp.concatenate([jnp.zeros((1,), jnp.int32), others.astype(jnp.int32)])
    shuffle = jax.random.permutation(jax.random.fold_in(base_key, 2), M_WIN)
    waves = chosen[shuffle]
    jitter = jax.random.randint(jax.random.fold_in(base_key, 3), (M_WIN,), 0, 4)
    jitter = jnp.where(waves == 0, 0, jitter)
    headroom = NT - waves
    shorten = jnp.minimum(8 * jitter, headroom // 2)
    return (waves.astype(jnp.int32), (headroom - shorten).astype(jnp.int32))


def draw_wave_ids(key, part):
    return wave_table(key)[0]


def draw_trunc_lengths(key, part):
    return wave_table(key)[1]


def draw_cycle_points(key, part):
    cycle_index = jnp.arange(NHALF, dtype=jnp.int32)
    jitter = jax.random.randint(jax.random.fold_in(key, 21), (NHALF,), 0, 4)
    northern = jnp.minimum(LONMAX, 20 + 4 * cycle_index + 4 * jitter)
    return jnp.concatenate([northern, northern[::-1]]).astype(jnp.int32)


def levels(key, extent, shards, least, high):
    def one(dim, blocks):
        heights = jax.random.uniform(jax.random.fold_in(jax.random.fold_in(key, 6), dim), (blocks,), jnp.float32, least / len(shards), high / len(shards))
        return jnp.repeat(jnp.exp(heights), extent[dim] // blocks).reshape((-1,) + (1,) * (len(extent) - dim - 1))

    gain = one(*shards[0])
    for cut in shards[1:]:
        gain = gain * one(*cut)
    return gain


def noise(stream_key, dims, width, bound, split=(), kind=jnp.bfloat16):
    values = width * jax.random.normal(stream_key, dims, jnp.float32)
    if split:
        values = values * levels(stream_key, dims, split, -0.22, 0.18)
    return jnp.clip(values, -bound, bound).astype(kind)


def setup_inputs(seed: int = 0) -> dict:
    keys = jax.random.split(jax.random.key(seed), 11)
    spectral = noise(keys[0], (M_WIN, 2 * FIELDS, LEVELS, NT), 0.002, 0.01171875, ((0, 32), (2, 8)))
    legendre = noise(keys[1], (M_WIN, NHALF, NT), 1.0, 4.0, ((0, 32),))
    wave_ids = draw_wave_ids(jax.random.fold_in(keys[10], 71), 0)
    trunc_lengths = draw_trunc_lengths(jax.random.fold_in(keys[10], 71), 0)
    cycle_points = draw_cycle_points(jax.random.fold_in(keys[10], 71), 0)
    grid_coef = noise(keys[5], (NLAT, LONMAX), 1.0, 6.0, ((0, 32),), jnp.float32)
    cycle_weights = jnp.clip(jnp.exp(jax.random.uniform(keys[6], (NHALF,), jnp.float32, math.log(0.1), math.log(2.0))), 0.1, 2.0)
    modes_in = noise(keys[7], (LEVELS, LEVELS), LEVELS ** -0.5, 0.5)
    modes_out = noise(keys[8], (LEVELS, LEVELS), LEVELS ** -0.5, 0.5)
    depths = jnp.clip(jnp.exp(jax.random.uniform(keys[9], (LEVELS,), jnp.float32, math.log(0.05), math.log(20.0))), 0.05, 20.0)
    return {"spectral": spectral, "legendre": legendre, "wave_ids": wave_ids, "trunc_lengths": trunc_lengths, "cycle_points": cycle_points, "grid_coef": grid_coef, "cycle_weights": cycle_weights, "modes_in": modes_in, "modes_out": modes_out, "depths": depths}


def trig_rows(wave_ids, cycle_count, lon_max):
    longitude = jnp.arange(lon_max, dtype=jnp.int32)
    counts = cycle_count[:, None, None]
    phase_idx = (wave_ids[None, :, None] * longitude[None, None, :]) % counts
    angles = (2.0 * jnp.pi) * phase_idx.astype(jnp.float32) / counts.astype(jnp.float32)
    live_mask = (longitude[None, None, :] < counts) & (2 * wave_ids[None, :, None] < counts)
    cosine = jnp.where(live_mask, jnp.cos(angles), 0.0)
    sine_part = jnp.where(live_mask, -jnp.sin(angles), 0.0)
    return jnp.stack([cosine, sine_part], axis=1).astype(jnp.bfloat16)


def cycle_trip(fourier, wave_ids, cycle_count, coef_rows):
    wave_total, channels, items, group_size = fourier.shape
    fields = channels // 2
    polys = trig_rows(wave_ids, cycle_count, coef_rows.shape[1])
    factor = jnp.where(wave_ids == 0, 1.0, 2.0).astype(jnp.bfloat16)
    weighted = (fourier * factor[:, None, None, None]).reshape(wave_total, 2, fields, items, group_size)
    grid_vals = jnp.einsum("mrfig,grmk->gfik", weighted.astype(jnp.float32), polys.astype(jnp.float32))
    tendency = (grid_vals * (coef_rows[:, None, None, :] + jnp.roll(grid_vals, -1, axis=1))).astype(jnp.bfloat16)
    analysed = jnp.einsum("gfik,grmk->mrfig", tendency.astype(jnp.float32), polys.astype(jnp.float32))
    analysed = analysed / cycle_count.astype(jnp.float32)
    return analysed.astype(jnp.bfloat16).reshape(wave_total, channels, items, group_size)


def reference(spectral, legendre, wave_ids, trunc_lengths, cycle_points, grid_coef, cycle_weights, modes_in, modes_out, depths):
    wave_total, channels, levels_total, spec_len = spectral.shape
    half_lat = legendre.shape[1]
    lat_total = 2 * half_lat
    position = jnp.arange(spec_len, dtype=jnp.int32)
    parity_sign = jnp.where(position % 2 == 0, 1.0, -1.0).astype(jnp.bfloat16)

    def inverse_one(packed):
        coeffs, polys, length = packed
        flat = coeffs.reshape(-1, spec_len)
        flat = jnp.where(position[None, :] < length, flat, jnp.zeros_like(flat))
        northern = jnp.dot(flat, polys.T, preferred_element_type=jnp.float32)
        southern = jnp.dot(flat * parity_sign[None, :], polys.T, preferred_element_type=jnp.float32)
        joined = jnp.concatenate([northern, jnp.flip(southern, axis=1)], axis=1).astype(jnp.bfloat16)
        return joined.reshape(channels, levels_total, lat_total)

    fourier = lax.map(inverse_one, (spectral, legendre, trunc_lengths))

    group_size = math.gcd(lat_total, 32)
    groups = lat_total // group_size
    stacked = jnp.moveaxis(fourier.reshape(wave_total, channels, levels_total, groups, group_size), 3, 0)
    counts = cycle_points.reshape(groups, group_size)
    coefs = grid_coef.reshape(groups, group_size, -1)

    def group_trip(packed):
        return cycle_trip(packed[0], wave_ids, packed[1], packed[2])

    results = lax.map(group_trip, (stacked, counts, coefs))
    returned = jnp.moveaxis(results, 0, 3).reshape(wave_total, channels, levels_total, lat_total)

    def forward_one(packed):
        values, polys, length, wavenum = packed
        northern = values[..., :half_lat].astype(jnp.float32)
        southern = jnp.flip(values[..., half_lat:], axis=2).astype(jnp.float32)
        even_part = (cycle_weights * (northern + southern)).astype(jnp.bfloat16).reshape(-1, half_lat)
        odd_part = (cycle_weights * (northern - southern)).astype(jnp.bfloat16).reshape(-1, half_lat)
        from_even = jnp.dot(even_part, polys, preferred_element_type=jnp.float32)
        from_odd = jnp.dot(odd_part, polys, preferred_element_type=jnp.float32)
        coeffs = jnp.where(position[None, :] % 2 == 0, from_even, from_odd)
        coeffs = jnp.where(position[None, :] < length, coeffs, 0.0).astype(jnp.bfloat16)
        coeffs = coeffs.reshape(channels, levels_total, spec_len)
        mode_vals = jnp.einsum("kl,cli->cki", modes_in.astype(jnp.float32), coeffs.astype(jnp.float32))
        degree = (wavenum + position).astype(jnp.float32)
        damp = 1.0 / (1.0 + depths[:, None] * degree[None, :] * (degree[None, :] + 1.0) / float(NT * NT))
        scaled = (mode_vals * damp[None, :, :]).astype(jnp.bfloat16)
        mixed = jnp.einsum("lk,cki->cli", modes_out.astype(jnp.float32), scaled.astype(jnp.float32))
        return mixed.astype(jnp.bfloat16)

    return lax.map(forward_one, (returned, legendre, trunc_lengths, wave_ids))
```

```python
import jax
import jax.numpy as jnp
import numpy as np
from jax import lax
from jax.experimental import pallas as pl
from jax.experimental.pallas import tpu as pltpu
from jax.sharding import PartitionSpec as P

MESH = pl.DeviceIdType.MESH
NT = 1280
BF = jnp.bfloat16
F32 = jnp.float32
WAVES = 32
LEVS = 8
DEVS = 256
CYC = 5
SECTIONS = ((0, 0, 0, 96), (0, 1, 96, 128), (1, 1, 0, 64), (1, 2, 64, 128), (2, 2, 0, 32), (2, 3, 32, 128))


def nt_dot(a, b):
    return lax.dot_general(a, b, (((1,), (1,)), ((), ())), preferred_element_type=F32)


def nn_dot(a, b):
    return lax.dot_general(a, b, (((1,), (0,)), ((), ())), preferred_element_type=F32)


def constant_arrays():
    block, row = np.divmod(np.arange(256), 16)
    tile, cyc = np.divmod(np.arange(240), 80)
    pack = (row[:, None] < 15) & (row[:, None] // 5 == tile[None]) & (5 * block[:, None] + row[:, None] % 5 == cyc[None])
    src_u, rest = np.divmod(np.arange(480), 96)
    src_t, src_w = np.divmod(rest, 32)
    in_w, in_row = np.divmod(np.arange(512), 16)
    unpack = (src_w[:, None] == in_w[None]) & (src_t[:, None] * 5 + src_u[:, None] == in_row[None])
    spread = np.arange(96)[:, None] == np.arange(384)[None] % 96
    fu, dest = np.divmod(np.arange(240), 16)
    back = (block[:, None] == dest[None]) & (row[:, None] == fu[None])
    return [x.astype(np.float32) for x in (pack, unpack, spread, back, pack.T, np.eye(256))]


def position():
    return lax.axis_index("wave"), lax.axis_index("lev")


def mirrored(dest):
    return jnp.where(dest < 128, dest, 383 - dest)


def inverse_rows(spec_ref, len_of, rhs):
    column = lax.broadcasted_iota(jnp.int32, (1, NT), 1)
    for idx, (t, m, lo, hi) in enumerate(SECTIONS):
        live = column < len_of(m)
        north = jnp.where(live, 1.0, 0.0).astype(BF)
        south = jnp.where(live, jnp.where(column % 2 == 0, 1.0, -1.0), 0.0).astype(BF)
        for half, factor in ((0, north), (128, south)):
            if lo > 0:
                rhs[idx, half : half + lo, :] = jnp.zeros((lo, NT), BF)
            if hi < 128:
                rhs[idx, half + hi : half + 128, :] = jnp.zeros((128 - hi, NT), BF)
            rhs[idx, half + lo : half + hi, :] = spec_ref[t * 128 + lo : t * 128 + hi, :] * factor


def inverse_dots(leg, rhs, waves_out):
    step = 320
    for t in range(3):
        ma, mb = SECTIONS[2 * t][1], SECTIONS[2 * t + 1][1]

        def block(jc, _):
            rows = pl.ds(pl.multiple_of(jc * step, 64), step)
            out = nt_dot(leg[ma, rows, :], rhs[2 * t]) + nt_dot(leg[mb, rows, :], rhs[2 * t + 1])
            waves_out[t, rows, :] = out.astype(BF)
            return 0

        lax.fori_loop(0, 640 // step, block, 0)


def inverse_pack(pack, waves_out, send):
    def block(g, _):
        rows = pl.ds(pl.multiple_of(g * 80, 16), 80)
        x = jnp.concatenate([waves_out[t, rows, :] for t in range(3)], axis=0)
        y = nn_dot(pack[...], x).astype(BF)
        send[pl.ds(g * 16, 16)] = y[:, :128].reshape(16, 16, 128)
        send[pl.ds(128 + g * 16, 16)] = y[:, 128:].reshape(16, 16, 128)
        return 0

    lax.fori_loop(0, 8, block, 0)


def cos_sin(steps, count):
    turns = jnp.round(steps * (4.0 / count))
    rest = steps - turns * (count * 0.25)
    x = rest * (2.0 * np.pi / count)
    x2 = x * x
    sine = x * (1.0 + x2 * (-1.0 / 6 + x2 * (1.0 / 120 + x2 * (-1.0 / 5040 + x2 * (1.0 / 362880)))))
    cosine = 1.0 + x2 * (-0.5 + x2 * (1.0 / 24 + x2 * (-1.0 / 720 + x2 * (1.0 / 40320))))
    quadrant = turns.astype(jnp.int32) & 3
    swap = (quadrant & 1) == 1
    c = jnp.where(swap, sine, cosine)
    s = jnp.where(swap, cosine, sine)
    c = jnp.where((quadrant == 1) | (quadrant == 2), -c, c)
    s = jnp.where(quadrant >= 2, -s, s)
    return c, s


def cycle_table(wave_col, points, table, low):
    count = jnp.full((1, 128), points, jnp.int32).astype(F32)
    lane = lax.broadcasted_iota(jnp.int32, (1, 128), 1)
    lane_f = lane.astype(F32)
    waves = wave_col[...]
    for half in range(2):
        c, s = cos_sin(waves * (lane_f + 128.0 * half), count)
        low[0, :, half * 128 : half * 128 + 128] = c
        low[1, :, half * 128 : half * 128 + 128] = s
    c_high, s_high = cos_sin(waves * (lane_f * 256.0), count)
    live = 2.0 * waves < count
    c_high = jnp.where(live, c_high, 0.0)
    s_high = jnp.where(live, s_high, 0.0)
    wide = lax.broadcasted_iota(jnp.int32, (1, 256), 1)
    for a in range(10):
        ca = c_high[:, a : a + 1]
        sa = s_high[:, a : a + 1]
        keep = jnp.where(wide + 256 * a < points, 1.0, 0.0)
        cl = low[0] * keep
        sl = low[1] * keep
        cols = slice(a * 256, a * 256 + 256)
        table[0:128, cols] = (cl * ca - sl * sa).astype(BF)
        table[128:256, cols] = (-(sl * ca + cl * sa)).astype(BF)


def gather_waves(recv, unpack, spread, wave_row, fields):
    lane = lax.broadcasted_iota(jnp.int32, (1, 384), 1)
    sections = [jnp.where((lane >= 96 * m) & (lane < 96 * m + 96), 1.0, 0.0).astype(BF) for m in range(4)]
    factor = jnp.where(wave_row[0:1, :] == 0.0, 1.0, 2.0)

    def pair(sp, _):
        first = recv[pl.ds(sp * 64, 32)].reshape(512, 128)
        second = recv[pl.ds(sp * 64 + 32, 32)].reshape(512, 128)
        z = nn_dot(unpack[...], jnp.concatenate([first, second], axis=1)).astype(BF)
        for u in range(CYC):
            pieces = []
            for h in range(2):
                zu = jnp.concatenate(
                    [z[u * 96 + t * 32 : u * 96 + t * 32 + 32, h * 128 : h * 128 + 128] for t in range(3)], axis=1
                )
                pieces += [zu * sections[m] for m in range(4)]
            y = nt_dot(spread[...], jnp.concatenate(pieces, axis=0))
            for h in range(2):
                part = (y[:, h * 128 : h * 128 + 128] * factor).astype(BF)
                for r in range(2):
                    for f in range(3):
                        rows = pl.ds(pl.multiple_of(f * 128 + sp * 32 + h * 16, 16), 16)
                        fields[u, rows, r * 128 : r * 128 + 128] = part[r * 48 + f * 16 : r * 48 + f * 16 + 16, :]
        return 0

    lax.fori_loop(0, 4, pair, 0)


def grid_cycle(u, points, coef_row, table, fields, tend, analysed):
    for a in range(10):
        cols = slice(a * 256, a * 256 + 256)
        g = nn_dot(fields[u], table[:, cols])
        coef = coef_row[:, cols]
        for f in range(3):
            nxt = (f + 1) % 3
            tend[f * 128 : f * 128 + 128, cols] = (
                g[f * 128 : f * 128 + 128] * (coef + g[nxt * 128 : nxt * 128 + 128])
            ).astype(BF)
    total = nt_dot(table[...], tend[...])
    count = jnp.full((1, 384), points, jnp.int32).astype(F32)
    analysed[u] = (total / count).astype(BF)


def pack_return(back, analysed, send):
    def pair(g, _):
        halves = []
        for h in range(2):
            rows = pl.ds(pl.multiple_of(g * 32 + h * 16, 16), 16)
            halves.append(
                jnp.concatenate(
                    [analysed[u, rows, f * 128 : f * 128 + 128] for f in range(3) for u in range(CYC)], axis=0
                )
            )
        y = nn_dot(back[...], jnp.concatenate(halves, axis=1)).astype(BF)
        send[pl.ds(g * 32, 16)] = y[:, :128].reshape(16, 16, 128)
        send[pl.ds(g * 32 + 16, 16)] = y[:, 128:].reshape(16, 16, 128)
        return 0

    lax.fori_loop(0, 8, pair, 0)


def parity_parts(recv, packt, weight_col, parts):
    def block(g, _):
        rows = pl.ds(pl.multiple_of(g * 80, 16), 80)
        x = jnp.concatenate(
            [recv[pl.ds(g * 16, 16)].reshape(256, 128), recv[pl.ds(128 + g * 16, 16)].reshape(256, 128)], axis=1
        )
        z = nn_dot(packt[...], x)
        weight = weight_col[rows, :]
        for f in range(3):
            north = z[f * 80 : f * 80 + 80, :128]
            south = z[f * 80 : f * 80 + 80, 128:]
            parts[f, rows, 0:128] = (weight * (north + south)).astype(BF)
            parts[f, rows, 128:256] = (weight * (north - south)).astype(BF)
        return 0

    lax.fori_loop(0, 8, block, 0)


def forward_modes(leg_m, length, wave, eye, parts, flipped, modes_in, modes_out, depth_col, update):
    for f in range(3):
        t = nt_dot(eye[...], parts[f]).astype(BF)
        flipped[0, f * 128 : f * 128 + 128, :] = t[:128]
        flipped[1, f * 128 : f * 128 + 128, :] = t[128:]
    lane = lax.broadcasted_iota(jnp.int32, (1, 256), 1)
    even_lane = lane % 2 == 0

    def block(ic, _):
        cols = pl.ds(pl.multiple_of(ic * 256, 256), 256)
        polys = leg_m(cols)
        even = nn_dot(flipped[0], polys)
        odd = nn_dot(flipped[1], polys)
        where = lane + ic * 256
        proj = jnp.where(where < length, jnp.where(even_lane, even, odd), 0.0).astype(BF)
        degree = (where + wave).astype(F32)
        depth = depth_col[:, 0:1]
        damp = 1.0 / (1.0 + depth * degree * (degree + 1.0) / float(NT * NT))
        for f in range(3):
            vals = nn_dot(modes_in[...], proj[f * 128 : f * 128 + 128])
            scaled = (vals * damp).astype(BF)
            update[f, :, cols] = nn_dot(modes_out[...], scaled).astype(BF)
        return 0

    lax.fori_loop(0, NT // 256, block, 0)


def kernel_inverse(lens, spec, leg, pack, send, rhs, waves_out):
    w, _ = position()
    inverse_rows(spec, lambda m: lens[w * 4 + m], rhs)
    inverse_dots(leg, rhs, waves_out)
    inverse_pack(pack, waves_out, send)


def kernel_grid(cyc, recv, coef, wave_col, wave_row, unpack, spread, back, send, table, low, fields, tend, analysed):
    w, s = position()
    dest = w * LEVS + s
    gather_waves(recv, unpack, spread, wave_row, fields)

    def cycle(u, _):
        shift = jnp.where(dest < 128, u, 4 - u)
        points = cyc[dest * CYC + shift]
        cycle_table(wave_col, points, table, low)
        grid_cycle(u, points, coef[pl.ds(s * CYC + shift, 1), :], table, fields, tend, analysed)
        return 0

    lax.fori_loop(0, CYC, cycle, 0)
    pack_return(back, analysed, send)


def kernel_forward(
    lens, waves, recv, leg, packt, eye, weight_col, modes_in, modes_out, depth_col, update, polys, parts, flipped, sem
):
    w, s = position()
    m = s // 2
    fetch = pltpu.make_async_copy(leg.at[m], polys, sem)
    fetch.start()
    parity_parts(recv, packt, weight_col, parts)
    fetch.wait()
    forward_modes(
        lambda cols: polys[:, cols],
        lens[w * 4 + m],
        waves[w * 4 + m],
        eye,
        parts,
        flipped,
        modes_in,
        modes_out,
        depth_col,
        update,
    )


def greet(first, second, everyone):
    w, s = position()

    def lev_peer(i, sem):
        pl.semaphore_signal(sem, inc=1, device_id=(w, lax.rem(s + i, LEVS)), device_id_type=MESH)
        return sem

    def wave_peer(i, sem):
        pl.semaphore_signal(sem, inc=1, device_id=(lax.rem(w + i, WAVES), s), device_id_type=MESH)
        return sem

    lax.fori_loop(1, LEVS, lambda i, c: (lev_peer(i, first), c)[1], 0)
    if not everyone:
        pl.semaphore_wait(first, LEVS - 1)
        return
    lax.fori_loop(1, WAVES, lambda i, c: (wave_peer(i, first), c)[1], 0)
    pl.semaphore_wait(first, LEVS - 1 + WAVES - 1)
    lax.fori_loop(1, WAVES, lambda i, c: (wave_peer(i, second), c)[1], 0)
    pl.semaphore_wait(second, WAVES - 1)


def exchange_all(send, recv, send_sem, recv_sem, own_sem, source_slot, my_slot):
    w, s = position()
    own = pltpu.make_async_copy(send.at[source_slot(w, s)], recv.at[my_slot], own_sem)
    own.start()

    def start(i, _):
        tw = lax.rem(w + lax.rem(i, WAVES), WAVES)
        ts = lax.rem(s + i // WAVES, LEVS)
        pltpu.make_async_remote_copy(
            src_ref=send.at[source_slot(tw, ts)],
            dst_ref=recv.at[my_slot],
            send_sem=send_sem,
            recv_sem=recv_sem,
            device_id=(tw, ts),
            device_id_type=MESH,
        ).start()
        return 0

    lax.fori_loop(1, DEVS, start, 0)
    own.wait()
    rest = pl.ds(0, DEVS - 1)
    pltpu.make_async_copy(send.at[rest], send.at[rest], send_sem).wait()
    pltpu.make_async_copy(recv.at[rest], recv.at[rest], recv_sem).wait()


def kernel_to_cycles(send, recv, second, send_sem, recv_sem, own_sem):
    w, s = position()
    greet(pltpu.get_barrier_semaphore(), second, True)
    exchange_all(send, recv, send_sem, recv_sem, own_sem, lambda tw, ts: mirrored(tw * LEVS + ts), s * WAVES + w)


def kernel_to_waves(send, recv, second, send_sem, recv_sem, own_sem):
    w, s = position()
    greet(pltpu.get_barrier_semaphore(), second, True)
    exchange_all(
        send,
        recv,
        send_sem,
        recv_sem,
        own_sem,
        lambda tw, ts: lax.rem(ts, 2) * 128 + (ts // 2) * 32 + tw,
        mirrored(w * LEVS + s),
    )


def kernel_to_levels(update, out, send_sem, recv_sem, own_sem):
    w, s = position()
    greet(pltpu.get_barrier_semaphore(), None, False)
    m, r = s // 2, lax.rem(s, 2)

    def piece(ts):
        return update.at[:, pl.ds(pl.multiple_of(ts * 16, 16), 16), :]

    place = out.at[m, pl.ds(r * 3, 3)]
    own = pltpu.make_async_copy(piece(s), place, own_sem)
    own.start()
    for i in range(1, LEVS):
        ts = lax.rem(s + i, LEVS)
        pltpu.make_async_remote_copy(
            src_ref=piece(ts),
            dst_ref=place,
            send_sem=send_sem.at[i - 1],
            recv_sem=recv_sem.at[i - 1],
            device_id=(w, ts),
            device_id_type=MESH,
        ).start()
    own.wait()
    for i in range(1, LEVS):
        done = pltpu.make_async_remote_copy(
            src_ref=piece(s),
            dst_ref=place,
            send_sem=send_sem.at[i - 1],
            recv_sem=recv_sem.at[i - 1],
            device_id=(w, lax.rem(s + i, LEVS)),
            device_id_type=MESH,
        )
        done.wait_send()
        done.wait_recv()


VM = pl.BlockSpec(memory_space=pltpu.VMEM)
SM = pl.BlockSpec(memory_space=pltpu.SMEM)
ANY = pl.BlockSpec(memory_space=pl.ANY)
LIMIT = 60 * 1024 * 1024


def call(kernel, ins, outs, out_shape, scratch, name, cid=None):
    extra = {} if cid is None else {"collective_id": cid, "has_side_effects": True}
    return pl.pallas_call(
        kernel,
        out_shape=out_shape,
        in_specs=ins,
        out_specs=outs,
        scratch_shapes=scratch,
        name=name,
        compiler_params=pltpu.CompilerParams(vmem_limit_bytes=LIMIT, **extra),
    )


MESSAGES = jax.ShapeDtypeStruct((DEVS, 16, 128), BF)
SEMS = [pltpu.SemaphoreType.REGULAR] + [pltpu.SemaphoreType.DMA] * 3


def inverse_call(lens, spec, leg, pack):
    return call(
        kernel_inverse,
        [SM, VM, VM, VM],
        VM,
        MESSAGES,
        [pltpu.VMEM((6, 256, NT), BF), pltpu.VMEM((3, 640, 256), BF)],
        "inverse",
    )(lens, spec, leg, pack)


def grid_call(cyc, recv, coef, wave_col, wave_row, unpack, spread, back):
    return call(
        kernel_grid,
        [SM] + [VM] * 7,
        VM,
        MESSAGES,
        [
            pltpu.VMEM((256, 2560), BF),
            pltpu.VMEM((2, 128, 256), F32),
            pltpu.VMEM((CYC, 384, 256), BF),
            pltpu.VMEM((384, 2560), BF),
            pltpu.VMEM((CYC, 256, 384), BF),
        ],
        "grid",
    )(cyc, recv, coef, wave_col, wave_row, unpack, spread, back)


def forward_call(lens, waves, recv, leg, packt, eye, weight_col, modes_in, modes_out, depth_col):
    return call(
        kernel_forward,
        [SM, SM, VM, ANY] + [VM] * 6,
        VM,
        jax.ShapeDtypeStruct((3, 128, NT), BF),
        [
            pltpu.VMEM((640, NT), BF),
            pltpu.VMEM((3, 640, 256), BF),
            pltpu.VMEM((2, 384, 640), BF),
            pltpu.SemaphoreType.DMA,
        ],
        "forward",
    )(lens, waves, recv, leg, packt, eye, weight_col, modes_in, modes_out, depth_col)


def side_arrays(wave_ids, cycle_weights, depths):
    order = wave_ids.reshape(32, 4).T.reshape(128).astype(F32)
    wave_col = jnp.broadcast_to(order[:, None], (128, 128))
    wave_row = jnp.broadcast_to(order[None, :], (8, 128))
    weight_col = jnp.broadcast_to(cycle_weights[:, None], (640, 128))
    depth_col = jnp.broadcast_to(depths[:, None], (128, 128))
    return wave_col, wave_row, weight_col, depth_col


def on_device(
    spectral,
    legendre,
    wave_ids,
    trunc_lengths,
    cycle_points,
    grid_coef,
    cycle_weights,
    modes_in,
    modes_out,
    depths,
):
    pack, unpack, spread, back, packt, eye = [jnp.asarray(x, BF) for x in constant_arrays()]
    wave_col, wave_row, weight_col, depth_col = side_arrays(wave_ids, cycle_weights, depths)
    send = inverse_call(trunc_lengths, spectral.reshape(384, NT), legendre, pack)
    recv = call(kernel_to_cycles, [VM], VM, MESSAGES, SEMS, "to_cycles", 0)(send)
    send = grid_call(cycle_points, recv, grid_coef, wave_col, wave_row, unpack, spread, back)
    recv = call(kernel_to_waves, [VM], VM, MESSAGES, SEMS, "to_waves", 1)(send)
    update = forward_call(
        trunc_lengths, wave_ids, recv, legendre, packt, eye, weight_col, modes_in, modes_out, depth_col
    )
    return call(
        kernel_to_levels,
        [VM],
        ANY,
        jax.ShapeDtypeStruct((4, 6, 16, NT), BF),
        [pltpu.SemaphoreType.DMA((LEVS - 1,)), pltpu.SemaphoreType.DMA((LEVS - 1,)), pltpu.SemaphoreType.DMA],
        "to_levels",
        2,
    )(update)


def solution(mesh):
    placed = (
        P("wave", None, "lev", None),
        P("wave", None, None),
        P(),
        P(),
        P(),
        P("wave", None),
        P(),
        P(),
        P(),
        P(),
    )
    return jax.shard_map(
        on_device,
        mesh=mesh,
        in_specs=placed,
        out_specs=P("wave", None, "lev", None),
        check_vma=False,
    )
```

```python
import jax
import jax.numpy as jnp
import numpy as np
from jax import lax
from jax.experimental import pallas as pl
from jax.experimental.pallas import tpu as pltpu
from jax.sharding import PartitionSpec as P

MESH = pl.DeviceIdType.MESH
NT = 1280
BF = jnp.bfloat16
F32 = jnp.float32
WAVES = 32
LEVS = 8
DEVS = 256
CYC = 5
SECTIONS = ((0, 0, 0, 96), (0, 1, 96, 128), (1, 1, 0, 64), (1, 2, 64, 128), (2, 2, 0, 32), (2, 3, 32, 128))


def nt_dot(a, b):
    return lax.dot_general(a, b, (((1,), (1,)), ((), ())), preferred_element_type=F32)


def nn_dot(a, b):
    return lax.dot_general(a, b, (((1,), (0,)), ((), ())), preferred_element_type=F32)


def constant_arrays():
    block, row = np.divmod(np.arange(256), 16)
    tile, cyc = np.divmod(np.arange(240), 80)
    pack = (row[:, None] < 15) & (row[:, None] // 5 == tile[None]) & (5 * block[:, None] + row[:, None] % 5 == cyc[None])
    src_u, rest = np.divmod(np.arange(480), 96)
    src_t, src_w = np.divmod(rest, 32)
    in_w, in_row = np.divmod(np.arange(512), 16)
    unpack = (src_w[:, None] == in_w[None]) & (src_t[:, None] * 5 + src_u[:, None] == in_row[None])
    spread = np.arange(96)[:, None] == np.arange(384)[None] % 96
    fu, dest = np.divmod(np.arange(240), 16)
    back = (block[:, None] == dest[None]) & (row[:, None] == fu[None])
    return [x.astype(np.float32) for x in (pack, unpack, spread, back, pack.T, np.eye(256))]


def position():
    return lax.axis_index("wave"), lax.axis_index("lev")


def shifted(dz, dy, dx, dc):
    w, s = position()
    tw = lax.rem(w // 4 + dz, 8) * 4 + lax.rem(w + dy, 4)
    return tw, lax.rem(s // 2 + dx, 4) * 2 + lax.rem(s + dc, 2)


def mirrored(dest):
    return jnp.where(dest < 128, dest, 383 - dest)


def inverse_rows(spec_ref, len_of, rhs):
    column = lax.broadcasted_iota(jnp.int32, (1, NT), 1)
    for idx, (t, m, lo, hi) in enumerate(SECTIONS):
        live = column < len_of(m)
        north = jnp.where(live, 1.0, 0.0).astype(BF)
        south = jnp.where(live, jnp.where(column % 2 == 0, 1.0, -1.0), 0.0).astype(BF)
        for half, factor in ((0, north), (128, south)):
            if lo > 0:
                rhs[idx, half : half + lo, :] = jnp.zeros((lo, NT), BF)
            if hi < 128:
                rhs[idx, half + hi : half + 128, :] = jnp.zeros((128 - hi, NT), BF)
            rhs[idx, half + lo : half + hi, :] = spec_ref[t * 128 + lo : t * 128 + hi, :] * factor


def inverse_dots(t, leg, rhs, waves_out):
    step = 320
    ma, mb = SECTIONS[2 * t][1], SECTIONS[2 * t + 1][1]

    def block(jc, _):
        rows = pl.ds(pl.multiple_of(jc * step, 64), step)
        out = nt_dot(leg[ma, rows, :], rhs[2 * t]) + nt_dot(leg[mb, rows, :], rhs[2 * t + 1])
        waves_out[t, rows, :] = out.astype(BF)
        return 0

    lax.fori_loop(0, 640 // step, block, 0)


def inverse_pack(pack, waves_out, send):
    def block(g, _):
        rows = pl.ds(pl.multiple_of(g * 80, 16), 80)
        x = jnp.concatenate([waves_out[t, rows, :] for t in range(3)], axis=0)
        y = nn_dot(pack[...], x).astype(BF)
        send[pl.ds(g * 16, 16)] = y[:, :128].reshape(16, 16, 128)
        send[pl.ds(128 + g * 16, 16)] = y[:, 128:].reshape(16, 16, 128)
        return 0

    lax.fori_loop(0, 8, block, 0)


def cos_sin(steps, count):
    turns = jnp.round(steps * (4.0 / count))
    rest = steps - turns * (count * 0.25)
    x = rest * (2.0 * np.pi / count)
    x2 = x * x
    sine = x * (1.0 + x2 * (-1.0 / 6 + x2 * (1.0 / 120 + x2 * (-1.0 / 5040 + x2 * (1.0 / 362880)))))
    cosine = 1.0 + x2 * (-0.5 + x2 * (1.0 / 24 + x2 * (-1.0 / 720 + x2 * (1.0 / 40320))))
    quadrant = turns.astype(jnp.int32) & 3
    swap = (quadrant & 1) == 1
    c = jnp.where(swap, sine, cosine)
    s = jnp.where(swap, cosine, sine)
    c = jnp.where((quadrant == 1) | (quadrant == 2), -c, c)
    s = jnp.where(quadrant >= 2, -s, s)
    return c, s


def cycle_table(u, wave_col, points, table, low):
    count = jnp.full((1, 128), points, jnp.int32).astype(F32)
    lane = lax.broadcasted_iota(jnp.int32, (1, 128), 1)
    lane_f = lane.astype(F32)
    waves = wave_col[...]
    for half in range(2):
        c, s = cos_sin(waves * (lane_f + 128.0 * half), count)
        low[0, :, half * 128 : half * 128 + 128] = c
        low[1, :, half * 128 : half * 128 + 128] = s
    c_high, s_high = cos_sin(waves * (lane_f * 256.0), count)
    live = 2.0 * waves < count
    c_high = jnp.where(live, c_high, 0.0)
    s_high = jnp.where(live, s_high, 0.0)
    wide = lax.broadcasted_iota(jnp.int32, (1, 256), 1)
    for a in range(10):
        ca = c_high[:, a : a + 1]
        sa = s_high[:, a : a + 1]
        keep = jnp.where(wide + 256 * a < points, 1.0, 0.0)
        cl = low[0] * keep
        sl = low[1] * keep
        cols = slice(a * 256, a * 256 + 256)
        table[u, 0:128, cols] = (cl * ca - sl * sa).astype(BF)
        table[u, 128:256, cols] = (-(sl * ca + cl * sa)).astype(BF)


def gather_waves(recv, unpack, spread, wave_row, fields):
    lane = lax.broadcasted_iota(jnp.int32, (1, 384), 1)
    sections = [jnp.where((lane >= 96 * m) & (lane < 96 * m + 96), 1.0, 0.0).astype(BF) for m in range(4)]
    factor = jnp.where(wave_row[0:1, :] == 0.0, 1.0, 2.0)

    def pair(sp, _):
        first = recv[pl.ds(sp * 64, 32)].reshape(512, 128)
        second = recv[pl.ds(sp * 64 + 32, 32)].reshape(512, 128)
        z = nn_dot(unpack[...], jnp.concatenate([first, second], axis=1)).astype(BF)
        for u in range(CYC):
            pieces = []
            for h in range(2):
                zu = jnp.concatenate(
                    [z[u * 96 + t * 32 : u * 96 + t * 32 + 32, h * 128 : h * 128 + 128] for t in range(3)], axis=1
                )
                pieces += [zu * sections[m] for m in range(4)]
            y = nt_dot(spread[...], jnp.concatenate(pieces, axis=0))
            for h in range(2):
                part = (y[:, h * 128 : h * 128 + 128] * factor).astype(BF)
                for r in range(2):
                    for f in range(3):
                        rows = pl.ds(pl.multiple_of(f * 128 + sp * 32 + h * 16, 16), 16)
                        fields[u, rows, r * 128 : r * 128 + 128] = part[r * 48 + f * 16 : r * 48 + f * 16 + 16, :]
        return 0

    lax.fori_loop(0, 4, pair, 0)


def grid_cycle(u, points, coef_row, table, fields, tend, analysed):
    for a in range(10):
        cols = slice(a * 256, a * 256 + 256)
        g = nn_dot(fields[u], table[u, :, cols])
        coef = coef_row[:, cols]
        for f in range(3):
            nxt = (f + 1) % 3
            tend[f * 128 : f * 128 + 128, cols] = (
                g[f * 128 : f * 128 + 128] * (coef + g[nxt * 128 : nxt * 128 + 128])
            ).astype(BF)
    total = nt_dot(table[u], tend[...])
    count = jnp.full((1, 384), points, jnp.int32).astype(F32)
    analysed[u] = (total / count).astype(BF)


def pack_return(back, analysed, send):
    def pair(g, _):
        halves = []
        for h in range(2):
            rows = pl.ds(pl.multiple_of(g * 32 + h * 16, 16), 16)
            halves.append(
                jnp.concatenate(
                    [analysed[u, rows, f * 128 : f * 128 + 128] for f in range(3) for u in range(CYC)], axis=0
                )
            )
        y = nn_dot(back[...], jnp.concatenate(halves, axis=1)).astype(BF)
        send[pl.ds(g * 32, 16)] = y[:, :128].reshape(16, 16, 128)
        send[pl.ds(g * 32 + 16, 16)] = y[:, 128:].reshape(16, 16, 128)
        return 0

    lax.fori_loop(0, 8, pair, 0)


def parity_parts(recv, packt, weight_col, parts):
    def block(g, _):
        rows = pl.ds(pl.multiple_of(g * 80, 16), 80)
        x = jnp.concatenate(
            [recv[pl.ds(g * 16, 16)].reshape(256, 128), recv[pl.ds(128 + g * 16, 16)].reshape(256, 128)], axis=1
        )
        z = nn_dot(packt[...], x)
        weight = weight_col[rows, :]
        for f in range(3):
            north = z[f * 80 : f * 80 + 80, :128]
            south = z[f * 80 : f * 80 + 80, 128:]
            parts[f, rows, 0:128] = (weight * (north + south)).astype(BF)
            parts[f, rows, 128:256] = (weight * (north - south)).astype(BF)
        return 0

    lax.fori_loop(0, 8, block, 0)


def forward_modes(leg_m, length, wave, eye, parts, flipped, modes_in, modes_out, depth_col, update):
    for f in range(3):
        t = nt_dot(eye[...], parts[f]).astype(BF)
        flipped[0, f * 128 : f * 128 + 128, :] = t[:128]
        flipped[1, f * 128 : f * 128 + 128, :] = t[128:]
    lane = lax.broadcasted_iota(jnp.int32, (1, 256), 1)
    even_lane = lane % 2 == 0

    def block(ic, _):
        cols = pl.ds(pl.multiple_of(ic * 256, 256), 256)
        polys = leg_m(cols)
        even = nn_dot(flipped[0], polys)
        odd = nn_dot(flipped[1], polys)
        where = lane + ic * 256
        proj = jnp.where(where < length, jnp.where(even_lane, even, odd), 0.0).astype(BF)
        degree = (where + wave).astype(F32)
        depth = depth_col[:, 0:1]
        damp = 1.0 / (1.0 + depth * degree * (degree + 1.0) / float(NT * NT))
        for f in range(3):
            vals = nn_dot(modes_in[...], proj[f * 128 : f * 128 + 128])
            scaled = (vals * damp).astype(BF)
            update[f, :, cols] = nn_dot(modes_out[...], scaled).astype(BF)
        return 0

    lax.fori_loop(0, NT // 256, block, 0)


def column_of(row):
    return jnp.transpose(jnp.broadcast_to(row, (128, 128)))


def side_columns(waves_row, weights_row, depths_row, wave_col, wave_row, weight_col, depth_col):
    place = lax.broadcasted_iota(jnp.int32, (128, 128), 0)
    slot = lax.broadcasted_iota(jnp.int32, (128, 128), 1)
    order = jnp.where((place % 32) * 4 + place // 32 == slot, 1.0, 0.0).astype(BF)
    rows = jnp.broadcast_to(waves_row[...], (128, 128))
    high = (rows // 32).astype(F32).astype(BF)
    low = (rows % 32).astype(F32).astype(BF)
    column = nt_dot(order, high) * 32.0 + nt_dot(order, low)
    wave_col[...] = column
    wave_row[...] = jnp.transpose(column)[0:8]
    for i in range(5):
        weight_col[i * 128 : i * 128 + 128, :] = column_of(weights_row[:, i * 128 : i * 128 + 128])
    depth_col[...] = column_of(depths_row[...])


def send_all(send, recv, send_sem, recv_sem, own_sem, source_slot, my_slot):
    w, s = position()
    pltpu.make_async_copy(send.at[source_slot(w, s)], recv.at[my_slot], own_sem).start()

    def start(i, _):
        tw = lax.rem(w + lax.rem(i, WAVES), WAVES)
        ts = lax.rem(s + i // WAVES, LEVS)
        pltpu.make_async_remote_copy(
            src_ref=send.at[source_slot(tw, ts)],
            dst_ref=recv.at[my_slot],
            send_sem=send_sem,
            recv_sem=recv_sem,
            device_id=(tw, ts),
            device_id_type=MESH,
        ).start()
        return 0

    lax.fori_loop(1, DEVS, start, 0)


def wait_all(send, recv, send_sem, recv_sem, own_sem):
    rest = pl.ds(0, DEVS - 1)
    pltpu.make_async_copy(send.at[0], recv.at[0], own_sem).wait()
    pltpu.make_async_copy(send.at[rest], send.at[rest], send_sem).wait()
    pltpu.make_async_copy(recv.at[rest], recv.at[rest], recv_sem).wait()


def signal_peers(sem, peers):
    for peer in peers:
        pl.semaphore_signal(sem, inc=1, device_id=shifted(*peer), device_id_type=MESH)


LEV_PEERS = [(0, 0, dx, dc) for dx in range(4) for dc in range(2) if dx or dc]
Y_PEERS = [(0, dy, 0, 0) for dy in range(1, 4)]
Z_PEERS = [(dz, 0, 0, 0) for dz in range(1, 8)]
N_LATE = 6


def whole(
    lens,
    waves,
    cyc,
    spec_hbm,
    leg_hbm,
    pack_hbm,
    coef_hbm,
    unpack_hbm,
    spread_hbm,
    back_hbm,
    packt_hbm,
    eye_hbm,
    waves_row,
    weights_row,
    depths_row,
    modes_in,
    modes_out,
    out,
    spec,
    leg,
    pack,
    coef,
    unpack,
    spread,
    back,
    packt,
    eye,
    rhs,
    waves_out,
    send_a,
    recv_a,
    table,
    low,
    fields,
    tend,
    analysed,
    send_b,
    recv_b,
    parts,
    flipped,
    update,
    wave_col,
    wave_row,
    weight_col,
    depth_col,
    load_sem,
    late_sem,
    y_sem,
    z_sem,
    sems_a,
    sems_b,
    sems_c,
):
    w, s = position()
    dest = w * LEVS + s
    m, r = s // 2, lax.rem(s, 2)
    barrier = pltpu.get_barrier_semaphore()

    loads = [pltpu.make_async_copy(spec_hbm, spec, load_sem.at[0])]
    loads += [pltpu.make_async_copy(leg_hbm.at[i], leg.at[i], load_sem.at[1 + i]) for i in range(4)]
    loads += [pltpu.make_async_copy(pack_hbm, pack, load_sem.at[5])]
    late = [
        pltpu.make_async_copy(a, b, late_sem.at[i])
        for i, (a, b) in enumerate(
            [
                (coef_hbm, coef),
                (unpack_hbm, unpack),
                (spread_hbm, spread),
                (back_hbm, back),
                (packt_hbm, packt),
                (eye_hbm, eye),
            ]
        )
    ]
    for copy in loads + late:
        copy.start()

    signal_peers(barrier, LEV_PEERS + Y_PEERS + Z_PEERS)
    loads[0].wait()
    inverse_rows(spec, lambda i: lens[w * 4 + i], rhs)
    loads[1].wait()
    loads[2].wait()
    inverse_dots(0, leg, rhs, waves_out)
    pl.semaphore_wait(barrier, len(LEV_PEERS + Y_PEERS + Z_PEERS))
    signal_peers(y_sem, Y_PEERS)
    loads[3].wait()
    inverse_dots(1, leg, rhs, waves_out)
    pl.semaphore_wait(y_sem, len(Y_PEERS))
    signal_peers(z_sem, Z_PEERS)
    loads[4].wait()
    inverse_dots(2, leg, rhs, waves_out)
    loads[5].wait()
    inverse_pack(pack, waves_out, send_a)
    pl.semaphore_wait(z_sem, len(Z_PEERS))

    a_sems = [sems_a.at[i] for i in range(3)]
    send_all(send_a, recv_a, *a_sems, lambda tw, ts: mirrored(tw * LEVS + ts), s * WAVES + w)

    side_columns(waves_row, weights_row, depths_row, wave_col, wave_row, weight_col, depth_col)

    def shift(u):
        return jnp.where(dest < 128, u, 4 - u)

    def make_table(u, _):
        cycle_table(u, wave_col, cyc[dest * CYC + shift(u)], table, low)
        return 0

    lax.fori_loop(0, CYC, make_table, 0)
    for copy in late:
        copy.wait()
    wait_all(send_a, recv_a, *a_sems)

    gather_waves(recv_a, unpack, spread, wave_row, fields)

    def cycle(u, _):
        points = cyc[dest * CYC + shift(u)]
        grid_cycle(u, points, coef[pl.ds(s * CYC + shift(u), 1), :], table, fields, tend, analysed)
        return 0

    lax.fori_loop(0, CYC, cycle, 0)
    pack_return(back, analysed, send_b)
    b_sems = [sems_b.at[i] for i in range(3)]
    send_all(
        send_b, recv_b, *b_sems, lambda tw, ts: lax.rem(ts, 2) * 128 + (ts // 2) * 32 + tw, mirrored(w * LEVS + s)
    )
    wait_all(send_b, recv_b, *b_sems)

    parity_parts(recv_b, packt, weight_col, parts)
    forward_modes(
        lambda cols: leg[m, :, cols],
        lens[w * 4 + m],
        waves[w * 4 + m],
        eye,
        parts,
        flipped,
        modes_in,
        modes_out,
        depth_col,
        update,
    )

    def piece(ts):
        return update.at[:, pl.ds(pl.multiple_of(ts * 16, 16), 16), :]

    place = out.at[m, pl.ds(r * 3, 3)]
    for i in range(1, LEVS):
        ts = lax.rem(s + i, LEVS)
        pltpu.make_async_remote_copy(
            src_ref=piece(ts),
            dst_ref=place,
            send_sem=sems_c.at[0],
            recv_sem=sems_c.at[1],
            device_id=(w, ts),
            device_id_type=MESH,
        ).start()
    pltpu.make_async_copy(piece(s), place, sems_c.at[1]).start()
    sent = update.at[:, 0:112, :]
    pltpu.make_async_copy(sent, sent, sems_c.at[0]).wait()
    pltpu.make_async_copy(out, out, sems_c.at[1]).wait()


VM = pl.BlockSpec(memory_space=pltpu.VMEM)
SM = pl.BlockSpec(memory_space=pltpu.SMEM)
ANY = pl.BlockSpec(memory_space=pl.ANY)


def on_device(
    spectral,
    legendre,
    wave_ids,
    trunc_lengths,
    cycle_points,
    grid_coef,
    cycle_weights,
    modes_in,
    modes_out,
    depths,
):
    pack, unpack, spread, back, packt, eye = [jnp.asarray(x, BF) for x in constant_arrays()]
    vmem = pltpu.VMEM
    return pl.pallas_call(
        whole,
        out_shape=jax.ShapeDtypeStruct((4, 6, 16, NT), BF),
        in_specs=[SM] * 3 + [ANY] * 9 + [VM] * 5,
        out_specs=ANY,
        scratch_shapes=[
            vmem((384, NT), BF),
            vmem((4, 640, NT), BF),
            vmem((256, 240), BF),
            vmem((40, 2560), F32),
            vmem((480, 512), BF),
            vmem((96, 384), BF),
            vmem((256, 240), BF),
            vmem((240, 256), BF),
            vmem((256, 256), BF),
            vmem((6, 256, NT), BF),
            vmem((3, 640, 256), BF),
            vmem((DEVS, 16, 128), BF),
            vmem((DEVS, 16, 128), BF),
            vmem((CYC, 256, 2560), BF),
            vmem((2, 128, 256), F32),
            vmem((CYC, 384, 256), BF),
            vmem((384, 2560), BF),
            vmem((CYC, 256, 384), BF),
            vmem((DEVS, 16, 128), BF),
            vmem((DEVS, 16, 128), BF),
            vmem((3, 640, 256), BF),
            vmem((2, 384, 640), BF),
            vmem((3, 128, NT), BF),
            vmem((128, 128), F32),
            vmem((8, 128), F32),
            vmem((640, 128), F32),
            vmem((128, 128), F32),
            pltpu.SemaphoreType.DMA((6,)),
            pltpu.SemaphoreType.DMA((N_LATE,)),
            pltpu.SemaphoreType.REGULAR,
            pltpu.SemaphoreType.REGULAR,
            pltpu.SemaphoreType.DMA((3,)),
            pltpu.SemaphoreType.DMA((3,)),
            pltpu.SemaphoreType.DMA((2,)),
        ],
        name="whole",
        compiler_params=pltpu.CompilerParams(
            vmem_limit_bytes=56 * 1024 * 1024, collective_id=0, has_side_effects=True
        ),
    )(
        trunc_lengths,
        wave_ids,
        cycle_points,
        spectral.reshape(384, NT),
        legendre,
        pack,
        grid_coef,
        unpack,
        spread,
        back,
        packt,
        eye,
        wave_ids.reshape(1, 128),
        cycle_weights.reshape(1, 640),
        depths.reshape(1, 128),
        modes_in,
        modes_out,
    )


def solution(mesh):
    placed = (
        P("wave", None, "lev", None),
        P("wave", None, None),
        P(),
        P(),
        P(),
        P("wave", None),
        P(),
        P(),
        P(),
        P(),
    )
    return jax.shard_map(
        on_device,
        mesh=mesh,
        in_specs=placed,
        out_specs=P("wave", None, "lev", None),
        check_vma=False,
    )
```

```python
import jax
import jax.numpy as jnp
import numpy as np
from jax import lax
from jax.experimental import pallas as pl
from jax.experimental.pallas import tpu as pltpu
from jax.sharding import PartitionSpec as P

MESH = pl.DeviceIdType.MESH
NT = 1280
BF = jnp.bfloat16
F32 = jnp.float32
WAVES = 32
LEVS = 8
DEVS = 256
CYC = 5
HALF = DEVS * 8
SECTIONS = ((0, 0, 0, 96), (0, 1, 96, 128), (1, 1, 0, 64), (1, 2, 64, 128), (2, 2, 0, 32), (2, 3, 32, 128))


def nt_dot(a, b):
    return lax.dot_general(a, b, (((1,), (1,)), ((), ())), preferred_element_type=F32)


def nn_dot(a, b):
    return lax.dot_general(a, b, (((1,), (0,)), ((), ())), preferred_element_type=F32)


def constant_arrays():
    half, rest = np.divmod(np.arange(256), 128)
    block, row = np.divmod(rest, 8)
    row = row + half * 8
    tile, cyc = np.divmod(np.arange(240), 80)
    pack = (row[:, None] < 15) & (row[:, None] % 3 == tile[None]) & (5 * block[:, None] + row[:, None] // 3 == cyc[None])
    out_row, out_w = np.divmod(np.arange(256), 32)
    in_w, in_row = np.divmod(np.arange(256), 8)
    unpack = (out_w[:, None] == in_w[None]) & (out_row[:, None] == in_row[None])
    spread = np.arange(96)[:, None] == np.arange(384)[None] % 96
    return [x.astype(np.float32) for x in (pack, unpack, spread, unpack.T, pack.T, np.eye(256))]


def position():
    return lax.axis_index("wave"), lax.axis_index("lev")


def shifted(dz, dy, dx, dc):
    w, s = position()
    tw = lax.rem(w // 4 + dz, 8) * 4 + lax.rem(w + dy, 4)
    return tw, lax.rem(s // 2 + dx, 4) * 2 + lax.rem(s + dc, 2)


def mirrored(dest):
    return jnp.where(dest < 128, dest, 383 - dest)


def inverse_rows(spec_ref, len_of, rhs):
    column = lax.broadcasted_iota(jnp.int32, (1, NT), 1)
    for idx, (t, m, lo, hi) in enumerate(SECTIONS):
        live = column < len_of(m)
        north = jnp.where(live, 1.0, 0.0).astype(BF)
        south = jnp.where(live, jnp.where(column % 2 == 0, 1.0, -1.0), 0.0).astype(BF)
        for half, factor in ((0, north), (128, south)):
            if lo > 0:
                rhs[idx, half : half + lo, :] = jnp.zeros((lo, NT), BF)
            if hi < 128:
                rhs[idx, half + hi : half + 128, :] = jnp.zeros((128 - hi, NT), BF)
            rhs[idx, half + lo : half + hi, :] = spec_ref[t * 128 + lo : t * 128 + hi, :] * factor


def inverse_dots(t, leg, rhs, waves_out):
    step = 320
    ma, mb = SECTIONS[2 * t][1], SECTIONS[2 * t + 1][1]

    def block(jc, _):
        rows = pl.ds(pl.multiple_of(jc * step, 64), step)
        out = nt_dot(leg[ma, rows, :], rhs[2 * t]) + nt_dot(leg[mb, rows, :], rhs[2 * t + 1])
        waves_out[t, rows, :] = out.astype(BF)
        return 0

    lax.fori_loop(0, 640 // step, block, 0)


def inverse_pack(pack, waves_out, send):
    def block(g, _):
        rows = pl.ds(pl.multiple_of(g * 80, 16), 80)
        x = jnp.concatenate([waves_out[t, rows, :] for t in range(3)], axis=0)
        y = nn_dot(pack[...], x).astype(BF)
        for half in range(2):
            for side in range(2):
                rows = pl.ds(pl.multiple_of(half * HALF + side * 1024 + g * 128, 128), 128)
                send[rows, :] = y[half * 128 : half * 128 + 128, side * 128 : side * 128 + 128]
        return 0

    lax.fori_loop(0, 8, block, 0)


def cos_sin(steps, count):
    turns = jnp.round(steps * (4.0 / count))
    rest = steps - turns * (count * 0.25)
    x = rest * (2.0 * np.pi / count)
    x2 = x * x
    sine = x * (1.0 + x2 * (-1.0 / 6 + x2 * (1.0 / 120 + x2 * (-1.0 / 5040 + x2 * (1.0 / 362880)))))
    cosine = 1.0 + x2 * (-0.5 + x2 * (1.0 / 24 + x2 * (-1.0 / 720 + x2 * (1.0 / 40320))))
    quadrant = turns.astype(jnp.int32) & 3
    swap = (quadrant & 1) == 1
    c = jnp.where(swap, sine, cosine)
    s = jnp.where(swap, cosine, sine)
    c = jnp.where((quadrant == 1) | (quadrant == 2), -c, c)
    s = jnp.where(quadrant >= 2, -s, s)
    return c, s


def cycle_table(u, wave_col, points, table, low):
    count = jnp.full((1, 128), points, jnp.int32).astype(F32)
    lane = lax.broadcasted_iota(jnp.int32, (1, 128), 1)
    lane_f = lane.astype(F32)
    waves = wave_col[...]
    for half in range(2):
        c, s = cos_sin(waves * (lane_f + 128.0 * half), count)
        low[0, :, half * 128 : half * 128 + 128] = c
        low[1, :, half * 128 : half * 128 + 128] = s
    c_high, s_high = cos_sin(waves * (lane_f * 256.0), count)
    live = 2.0 * waves < count
    c_high = jnp.where(live, c_high, 0.0)
    s_high = jnp.where(live, s_high, 0.0)
    wide = lax.broadcasted_iota(jnp.int32, (1, 256), 1)
    for a in range(10):
        ca = c_high[:, a : a + 1]
        sa = s_high[:, a : a + 1]
        keep = jnp.where(wide + 256 * a < points, 1.0, 0.0)
        cl = low[0] * keep
        sl = low[1] * keep
        cols = slice(a * 256, a * 256 + 256)
        table[u, 0:128, cols] = (cl * ca - sl * sa).astype(BF)
        table[u, 128:256, cols] = (-(sl * ca + cl * sa)).astype(BF)


def gather_waves(half, recv, unpack, spread, wave_row, split, fields):
    lane = lax.broadcasted_iota(jnp.int32, (1, 384), 1)
    sections = [jnp.where((lane >= 96 * m) & (lane < 96 * m + 96), 1.0, 0.0).astype(BF) for m in range(4)]
    factor = jnp.where(wave_row[0:1, :] == 0.0, 1.0, 2.0)

    def pair(sp, _):
        first = recv[pl.ds(pl.multiple_of(half * HALF + sp * 512, 256), 256), :]
        second = recv[pl.ds(pl.multiple_of(half * HALF + sp * 512 + 256, 256), 256), :]
        z = nn_dot(unpack[...], jnp.concatenate([first, second], axis=1)).astype(BF)
        if half == 0:
            split[sp] = z[192:256]
            rows_of = {u: [z[96 * u + 32 * t : 96 * u + 32 * t + 32] for t in range(3)] for u in (0, 1)}
        else:
            rows_of = {u: [z[96 * u - 256 + 32 * t : 96 * u - 224 + 32 * t] for t in range(3)] for u in (3, 4)}
            rows_of[2] = [split[sp, 0:32], split[sp, 32:64], z[0:32]]
        for u, tiles in rows_of.items():
            pieces = []
            for h in range(2):
                zu = jnp.concatenate([x[:, h * 128 : h * 128 + 128] for x in tiles], axis=1)
                pieces += [zu * sections[m] for m in range(4)]
            y = nt_dot(spread[...], jnp.concatenate(pieces, axis=0))
            for h in range(2):
                part = (y[:, h * 128 : h * 128 + 128] * factor).astype(BF)
                for r in range(2):
                    for f in range(3):
                        rows = pl.ds(pl.multiple_of(f * 128 + sp * 32 + h * 16, 16), 16)
                        fields[u, rows, r * 128 : r * 128 + 128] = part[r * 48 + f * 16 : r * 48 + f * 16 + 16, :]
        return 0

    lax.fori_loop(0, 4, pair, 0)


def grid_cycle(u, points, coef_row, table, fields, tend, analysed):
    for a in range(10):
        cols = slice(a * 256, a * 256 + 256)
        g = nn_dot(fields[u], table[u, :, cols])
        coef = coef_row[:, cols]
        for f in range(3):
            nxt = (f + 1) % 3
            tend[f * 128 : f * 128 + 128, cols] = (
                g[f * 128 : f * 128 + 128] * (coef + g[nxt * 128 : nxt * 128 + 128])
            ).astype(BF)
    total = nt_dot(table[u], tend[...])
    count = jnp.full((1, 384), points, jnp.int32).astype(F32)
    analysed[u] = (total / count).astype(BF)


def pack_return(half, back, analysed, send):
    places = [divmod(half * 8 + i, 3) for i in range(8)]

    def pair(g, _):
        groups = []
        for h in range(2):
            rows = pl.ds(pl.multiple_of(g * 64 + h * 32, 32), 32)
            groups.append(
                jnp.concatenate(
                    [
                        analysed[u, rows, f * 128 : f * 128 + 128] if u < CYC else jnp.zeros((32, 128), BF)
                        for u, f in places
                    ],
                    axis=0,
                )
            )
        y = nn_dot(back[...], jnp.concatenate(groups, axis=1)).astype(BF)
        for h in range(2):
            rows = pl.ds(pl.multiple_of(half * HALF + g * 512 + h * 256, 256), 256)
            send[rows, :] = y[:, h * 128 : h * 128 + 128]
        return 0

    lax.fori_loop(0, 4, pair, 0)


def parity_parts(recv, packt, weight_col, parts):
    def block(g, _):
        rows = pl.ds(pl.multiple_of(g * 80, 16), 80)
        sides = []
        for side in range(2):
            starts = [pl.multiple_of(half * HALF + side * 1024 + g * 128, 128) for half in range(2)]
            sides.append(jnp.concatenate([recv[pl.ds(x, 128), :] for x in starts], axis=0))
        x = jnp.concatenate(sides, axis=1)
        z = nn_dot(packt[...], x)
        weight = weight_col[rows, :]
        for f in range(3):
            north = z[f * 80 : f * 80 + 80, :128]
            south = z[f * 80 : f * 80 + 80, 128:]
            parts[f, rows, 0:128] = (weight * (north + south)).astype(BF)
            parts[f, rows, 128:256] = (weight * (north - south)).astype(BF)
        return 0

    lax.fori_loop(0, 8, block, 0)


def forward_modes(leg_m, length, wave, eye, parts, flipped, modes_in, modes_out, depth_col, update, ready):
    for f in range(3):
        t = nt_dot(eye[...], parts[f]).astype(BF)
        flipped[0, f * 128 : f * 128 + 128, :] = t[:128]
        flipped[1, f * 128 : f * 128 + 128, :] = t[128:]
    lane = lax.broadcasted_iota(jnp.int32, (1, 256), 1)
    even_lane = lane % 2 == 0

    def block(ic, _):
        cols = pl.ds(pl.multiple_of(ic * 256, 256), 256)
        polys = leg_m(cols)
        even = nn_dot(flipped[0], polys)
        odd = nn_dot(flipped[1], polys)
        where = lane + ic * 256
        proj = jnp.where(where < length, jnp.where(even_lane, even, odd), 0.0).astype(BF)
        degree = (where + wave).astype(F32)
        depth = depth_col[:, 0:1]
        damp = 1.0 / (1.0 + depth * degree * (degree + 1.0) / float(NT * NT))
        for f in range(3):
            vals = nn_dot(modes_in[...], proj[f * 128 : f * 128 + 128])
            scaled = (vals * damp).astype(BF)
            update[f, :, cols] = nn_dot(modes_out[...], scaled).astype(BF)
        if ready is not None:

            @pl.when(ic > 0)
            def _():
                ready(ic - 1)

        return 0

    lax.fori_loop(0, NT // 256, block, 0)
    if ready is not None:
        ready(NT // 256 - 1)


def column_of(row):
    return jnp.transpose(jnp.broadcast_to(row, (128, 128)))


def side_columns(waves_row, weights, depths_row, wave_col, wave_row, weight_col, depth_col):
    place = lax.broadcasted_iota(jnp.int32, (128, 128), 0)
    slot = lax.broadcasted_iota(jnp.int32, (128, 128), 1)
    order = jnp.where((place % 32) * 4 + place // 32 == slot, 1.0, 0.0).astype(BF)
    rows = jnp.broadcast_to(waves_row[...], (128, 128))
    high = (rows // 32).astype(F32).astype(BF)
    low = (rows % 32).astype(F32).astype(BF)
    column = nt_dot(order, high) * 32.0 + nt_dot(order, low)
    wave_col[...] = column
    wave_row[...] = jnp.transpose(column)[0:8]
    for i in range(5):
        weight_col[i * 128 : i * 128 + 128, :] = column_of(weights[i : i + 1, :])
    depth_col[...] = column_of(depths_row[...])


def send_half(half, send, recv, sems, source_slot, my_slot):
    w, s = position()

    def rows(slot):
        return pl.ds(pl.multiple_of(half * HALF + slot * 8, 8), 8)

    pltpu.make_async_copy(send.at[rows(source_slot(w, s))], recv.at[rows(my_slot)], sems.at[half, 0]).start()

    def start(i, _):
        tw = lax.rem(w + lax.rem(i, WAVES), WAVES)
        ts = lax.rem(s + i // WAVES, LEVS)
        pltpu.make_async_remote_copy(
            src_ref=send.at[rows(source_slot(tw, ts))],
            dst_ref=recv.at[rows(my_slot)],
            send_sem=sems.at[half, 1],
            recv_sem=sems.at[half, 2],
            device_id=(tw, ts),
            device_id_type=MESH,
        ).start()
        return 0

    lax.fori_loop(1, DEVS, start, 0)


def wait_half(half, send, recv, sems):
    rest = pl.ds(half * HALF, HALF - 8)
    block = pl.ds(half * HALF, 8)
    pltpu.make_async_copy(send.at[block], recv.at[block], sems.at[half, 0]).wait()
    pltpu.make_async_copy(recv.at[rest], recv.at[rest], sems.at[half, 2]).wait()


def wait_sent(half, send, sems):
    rest = pl.ds(half * HALF, HALF - 8)
    pltpu.make_async_copy(send.at[rest], send.at[rest], sems.at[half, 1]).wait()


def signal_peers(sem, peers):
    for peer in peers:
        pl.semaphore_signal(sem, inc=1, device_id=shifted(*peer), device_id_type=MESH)


LEV_PEERS = [(0, 0, dx, dc) for dx in range(4) for dc in range(2) if dx or dc]
Y_PEERS = [(0, dy, 0, 0) for dy in range(1, 4)]
Z_PEERS = [(dz, 0, 0, 0) for dz in range(1, 8)]
N_LATE = 11


def whole(
    lens,
    waves,
    cyc,
    spec_hbm,
    leg_hbm,
    pack_hbm,
    coef_hbm,
    unpack_hbm,
    spread_hbm,
    back_hbm,
    packt_hbm,
    eye_hbm,
    weights_hbm,
    waves_row,
    depths_row,
    modes_in,
    modes_out,
    out,
    spec,
    leg,
    pack,
    coef,
    unpack,
    spread,
    back,
    packt,
    eye,
    rhs,
    waves_out,
    send_a,
    recv_a,
    split,
    table,
    low,
    fields,
    tend,
    analysed,
    send_b,
    recv_b,
    parts,
    flipped,
    update,
    wave_col,
    wave_row,
    weight_col,
    depth_col,
    weights,
    load_sem,
    late_sem,
    y_sem,
    z_sem,
    sems_a,
    sems_b,
    sems_c,
):
    w, s = position()
    dest = w * LEVS + s
    m, r = s // 2, lax.rem(s, 2)
    barrier = pltpu.get_barrier_semaphore()

    loads = [pltpu.make_async_copy(spec_hbm, spec, load_sem.at[0])]
    loads += [pltpu.make_async_copy(leg_hbm.at[i], leg.at[i], load_sem.at[1 + i]) for i in range(4)]
    loads += [pltpu.make_async_copy(pack_hbm, pack, load_sem.at[5])]
    late = [
        pltpu.make_async_copy(a, b, late_sem.at[i])
        for i, (a, b) in enumerate(
            [
                (coef_hbm, coef),
                (unpack_hbm, unpack),
                (spread_hbm, spread),
                (back_hbm, back),
                (packt_hbm, packt),
                (eye_hbm, eye),
                *[(weights_hbm.at[pl.ds(i * 128, 128)], weights.at[i]) for i in range(5)],
            ]
        )
    ]
    for copy in loads + late:
        copy.start()

    signal_peers(barrier, LEV_PEERS + Y_PEERS + Z_PEERS)
    loads[0].wait()
    inverse_rows(spec, lambda i: lens[w * 4 + i], rhs)
    loads[1].wait()
    loads[2].wait()
    inverse_dots(0, leg, rhs, waves_out)
    pl.semaphore_wait(barrier, len(LEV_PEERS + Y_PEERS + Z_PEERS))
    signal_peers(y_sem, Y_PEERS)
    loads[3].wait()
    inverse_dots(1, leg, rhs, waves_out)
    pl.semaphore_wait(y_sem, len(Y_PEERS))
    signal_peers(z_sem, Z_PEERS)
    loads[4].wait()
    inverse_dots(2, leg, rhs, waves_out)
    loads[5].wait()
    inverse_pack(pack, waves_out, send_a)
    pl.semaphore_wait(z_sem, len(Z_PEERS))

    for half in range(2):
        send_half(half, send_a, recv_a, sems_a, lambda tw, ts: mirrored(tw * LEVS + ts), s * WAVES + w)

    for copy in late:
        copy.wait()
    side_columns(waves_row, weights, depths_row, wave_col, wave_row, weight_col, depth_col)

    def shift(u):
        return jnp.where(dest < 128, u, 4 - u)

    def make_table(u, _):
        cycle_table(u, wave_col, cyc[dest * CYC + shift(u)], table, low)
        return 0

    lax.fori_loop(0, CYC, make_table, 0)

    def cycle(u, _):
        points = cyc[dest * CYC + shift(u)]
        grid_cycle(u, points, coef[pl.ds(s * CYC + shift(u), 1), :], table, fields, tend, analysed)
        return 0

    def return_half(half):
        pack_return(half, back, analysed, send_b)
        send_half(
            half,
            send_b,
            recv_b,
            sems_b,
            lambda tw, ts: lax.rem(ts, 2) * 128 + (ts // 2) * 32 + tw,
            mirrored(w * LEVS + s),
        )

    wait_half(0, send_a, recv_a, sems_a)
    gather_waves(0, recv_a, unpack, spread, wave_row, split, fields)
    lax.fori_loop(0, 2, cycle, 0)
    wait_half(1, send_a, recv_a, sems_a)
    gather_waves(1, recv_a, unpack, spread, wave_row, split, fields)
    cycle(2, 0)
    return_half(0)
    lax.fori_loop(3, CYC, cycle, 0)
    return_half(1)
    for half in range(2):
        wait_sent(half, send_a, sems_a)
        wait_half(half, send_b, recv_b, sems_b)
        wait_sent(half, send_b, sems_b)

    def to_levels(ic):
        cols = pl.ds(pl.multiple_of(ic * 256, 256), 256)
        place = out.at[m, pl.ds(r * 3, 3), :, cols]

        def piece(ts):
            return update.at[:, pl.ds(pl.multiple_of(ts * 16, 16), 16), cols]

        for i in range(1, LEVS):
            ts = lax.rem(s + i, LEVS)
            pltpu.make_async_remote_copy(
                src_ref=piece(ts),
                dst_ref=place,
                send_sem=sems_c.at[0],
                recv_sem=sems_c.at[1],
                device_id=(w, ts),
                device_id_type=MESH,
            ).start()
        pltpu.make_async_copy(piece(s), place, sems_c.at[1]).start()

    parity_parts(recv_b, packt, weight_col, parts)
    forward_modes(
        lambda cols: leg[m, :, cols],
        lens[w * 4 + m],
        waves[w * 4 + m],
        eye,
        parts,
        flipped,
        modes_in,
        modes_out,
        depth_col,
        update,
        to_levels,
    )
    sent = update.at[:, 0:112, :]
    pltpu.make_async_copy(sent, sent, sems_c.at[0]).wait()
    pltpu.make_async_copy(out, out, sems_c.at[1]).wait()


VM = pl.BlockSpec(memory_space=pltpu.VMEM)
SM = pl.BlockSpec(memory_space=pltpu.SMEM)
ANY = pl.BlockSpec(memory_space=pl.ANY)


def on_device(
    spectral,
    legendre,
    wave_ids,
    trunc_lengths,
    cycle_points,
    grid_coef,
    cycle_weights,
    modes_in,
    modes_out,
    depths,
):
    pack, unpack, spread, back, packt, eye = [jnp.asarray(x, BF) for x in constant_arrays()]
    vmem = pltpu.VMEM
    return pl.pallas_call(
        whole,
        out_shape=pltpu.VMEM((4, 6, 16, NT), BF),
        in_specs=[SM] * 3 + [ANY] * 10 + [VM] * 4,
        out_specs=VM,
        scratch_shapes=[
            vmem((384, NT), BF),
            vmem((4, 640, NT), BF),
            vmem((256, 240), BF),
            vmem((40, 2560), F32),
            vmem((256, 256), BF),
            vmem((96, 384), BF),
            vmem((256, 256), BF),
            vmem((240, 256), BF),
            vmem((256, 256), BF),
            vmem((6, 256, NT), BF),
            vmem((3, 640, 256), BF),
            vmem((2 * HALF, 128), BF),
            vmem((2 * HALF, 128), BF),
            vmem((4, 64, 256), BF),
            vmem((CYC, 256, 2560), BF),
            vmem((2, 128, 256), F32),
            vmem((CYC, 384, 256), BF),
            vmem((384, 2560), BF),
            vmem((CYC, 256, 384), BF),
            vmem((2 * HALF, 128), BF),
            vmem((2 * HALF, 128), BF),
            vmem((3, 640, 256), BF),
            vmem((2, 384, 640), BF),
            vmem((3, 128, NT), BF),
            vmem((128, 128), F32),
            vmem((8, 128), F32),
            vmem((640, 128), F32),
            vmem((128, 128), F32),
            vmem((8, 128), F32),
            pltpu.SemaphoreType.DMA((6,)),
            pltpu.SemaphoreType.DMA((N_LATE,)),
            pltpu.SemaphoreType.REGULAR,
            pltpu.SemaphoreType.REGULAR,
            pltpu.SemaphoreType.DMA((2, 3)),
            pltpu.SemaphoreType.DMA((2, 3)),
            pltpu.SemaphoreType.DMA((2,)),
        ],
        name="whole",
        compiler_params=pltpu.CompilerParams(
            vmem_limit_bytes=56 * 1024 * 1024, collective_id=0, has_side_effects=True
        ),
    )(
        trunc_lengths,
        wave_ids,
        cycle_points,
        spectral.reshape(384, NT),
        legendre,
        pack,
        grid_coef,
        unpack,
        spread,
        back,
        packt,
        eye,
        cycle_weights,
        wave_ids.reshape(1, 128),
        depths.reshape(1, 128),
        modes_in,
        modes_out,
    )


def solution(mesh):
    placed = (
        P("wave", None, "lev", None),
        P("wave", None, None),
        P(),
        P(),
        P(),
        P("wave", None),
        P(),
        P(),
        P(),
        P(),
    )
    return jax.shard_map(
        on_device,
        mesh=mesh,
        in_specs=placed,
        out_specs=P("wave", None, "lev", None),
        check_vma=False,
    )
```

```python
import jax
import jax.numpy as jnp
import numpy as np
from jax import lax
from jax.experimental import pallas as pl
from jax.experimental.pallas import tpu as pltpu
from jax.sharding import PartitionSpec as P

MESH = pl.DeviceIdType.MESH
NT = 1280
BF = jnp.bfloat16
F32 = jnp.float32
WAVES = 32
LEVS = 8
DEVS = 256
CYC = 5
HALF = DEVS * 8
SECTIONS = ((0, 0, 0, 96), (0, 1, 96, 128), (1, 1, 0, 64), (1, 2, 64, 128), (2, 2, 0, 32), (2, 3, 32, 128))


def nt_dot(a, b):
    return lax.dot_general(a, b, (((1,), (1,)), ((), ())), preferred_element_type=F32)


def nn_dot(a, b):
    return lax.dot_general(a, b, (((1,), (0,)), ((), ())), preferred_element_type=F32)


def constant_arrays():
    half, rest = np.divmod(np.arange(256), 128)
    block, row = np.divmod(rest, 8)
    row = row + half * 8
    tile, cyc = np.divmod(np.arange(240), 80)
    pack = (row[:, None] < 15) & (row[:, None] % 3 == tile[None]) & (5 * block[:, None] + row[:, None] // 3 == cyc[None])
    out_row, out_w = np.divmod(np.arange(256), 32)
    in_w, in_row = np.divmod(np.arange(256), 8)
    unpack = (out_w[:, None] == in_w[None]) & (out_row[:, None] == in_row[None])
    spread = np.arange(96)[:, None] == np.arange(384)[None] % 96
    return [x.astype(np.float32) for x in (pack, unpack, spread, unpack.T, pack.T, np.eye(256))]


def position():
    return lax.axis_index("wave"), lax.axis_index("lev")


def shifted(dz, dy, dx, dc):
    w, s = position()
    tw = lax.rem(w // 4 + dz, 8) * 4 + lax.rem(w + dy, 4)
    return tw, lax.rem(s // 2 + dx, 4) * 2 + lax.rem(s + dc, 2)


def mirrored(dest):
    return jnp.where(dest < 128, dest, 383 - dest)


def inverse_rows(spec_ref, len_of, rhs):
    column = lax.broadcasted_iota(jnp.int32, (1, NT), 1)
    for idx, (t, m, lo, hi) in enumerate(SECTIONS):
        live = column < len_of(m)
        north = jnp.where(live, 1.0, 0.0).astype(BF)
        south = jnp.where(live, jnp.where(column % 2 == 0, 1.0, -1.0), 0.0).astype(BF)
        for half, factor in ((0, north), (128, south)):
            if lo > 0:
                rhs[idx, half : half + lo, :] = jnp.zeros((lo, NT), BF)
            if hi < 128:
                rhs[idx, half + hi : half + 128, :] = jnp.zeros((128 - hi, NT), BF)
            rhs[idx, half + lo : half + hi, :] = spec_ref[t * 128 + lo : t * 128 + hi, :] * factor


def inverse_dots(t, leg, rhs, waves_out):
    step = 320
    ma, mb = SECTIONS[2 * t][1], SECTIONS[2 * t + 1][1]

    def block(jc, _):
        rows = pl.ds(pl.multiple_of(jc * step, 64), step)
        out = nt_dot(leg[ma, rows, :], rhs[2 * t]) + nt_dot(leg[mb, rows, :], rhs[2 * t + 1])
        waves_out[t, rows, :] = out.astype(BF)
        return 0

    lax.fori_loop(0, 640 // step, block, 0)


def inverse_pack(pack, waves_out, send):
    def block(g, _):
        rows = pl.ds(pl.multiple_of(g * 80, 16), 80)
        x = jnp.concatenate([waves_out[t, rows, :] for t in range(3)], axis=0)
        y = nn_dot(pack[...], x).astype(BF)
        for half in range(2):
            for side in range(2):
                rows = pl.ds(pl.multiple_of(half * HALF + side * 1024 + g * 128, 128), 128)
                send[rows, :] = y[half * 128 : half * 128 + 128, side * 128 : side * 128 + 128]
        return 0

    lax.fori_loop(0, 8, block, 0, unroll=4)


def cos_sin(steps, count):
    turns = jnp.round(steps * (4.0 / count))
    rest = steps - turns * (count * 0.25)
    x = rest * (2.0 * np.pi / count)
    x2 = x * x
    sine = x * (1.0 + x2 * (-1.0 / 6 + x2 * (1.0 / 120 + x2 * (-1.0 / 5040 + x2 * (1.0 / 362880)))))
    cosine = 1.0 + x2 * (-0.5 + x2 * (1.0 / 24 + x2 * (-1.0 / 720 + x2 * (1.0 / 40320))))
    quadrant = turns.astype(jnp.int32) & 3
    swap = (quadrant & 1) == 1
    c = jnp.where(swap, sine, cosine)
    s = jnp.where(swap, cosine, sine)
    c = jnp.where((quadrant == 1) | (quadrant == 2), -c, c)
    s = jnp.where(quadrant >= 2, -s, s)
    return c, s


def cycle_table(u, wave_col, points, table, low):
    count = jnp.full((1, 128), points, jnp.int32).astype(F32)
    lane = lax.broadcasted_iota(jnp.int32, (1, 128), 1)
    lane_f = lane.astype(F32)
    waves = wave_col[...]
    for half in range(2):
        c, s = cos_sin(waves * (lane_f + 128.0 * half), count)
        low[0, :, half * 128 : half * 128 + 128] = c
        low[1, :, half * 128 : half * 128 + 128] = s
    c_high, s_high = cos_sin(waves * (lane_f * 256.0), count)
    live = 2.0 * waves < count
    c_high = jnp.where(live, c_high, 0.0)
    s_high = jnp.where(live, s_high, 0.0)
    wide = lax.broadcasted_iota(jnp.int32, (1, 256), 1)
    for a in range(10):
        ca = c_high[:, a : a + 1]
        sa = s_high[:, a : a + 1]
        keep = jnp.where(wide + 256 * a < points, 1.0, 0.0)
        cl = low[0] * keep
        sl = low[1] * keep
        cols = slice(a * 256, a * 256 + 256)
        table[u, 0:128, cols] = (cl * ca - sl * sa).astype(BF)
        table[u, 128:256, cols] = (-(sl * ca + cl * sa)).astype(BF)


def gather_waves(cycles, recv, unpack, spread, wave_row, split, fields):
    lane = lax.broadcasted_iota(jnp.int32, (1, 384), 1)
    sections = [jnp.where((lane >= 96 * m) & (lane < 96 * m + 96), 1.0, 0.0).astype(BF) for m in range(4)]
    factor = jnp.where(wave_row[0:1, :] == 0.0, 1.0, 2.0)

    def pair(sp, _):
        def sorted_half(half):
            starts = [pl.multiple_of(half * HALF + sp * 512 + h * 256, 256) for h in range(2)]
            return nn_dot(unpack[...], jnp.concatenate([recv[pl.ds(x, 256), :] for x in starts], axis=1)).astype(BF)

        if cycles == (0, 1):
            z = sorted_half(0)
            split[sp, 0:64] = z[192:256]
            rows_of = {u: [z[96 * u + 32 * t : 96 * u + 32 * t + 32] for t in range(3)] for u in cycles}
        elif cycles == (2,):
            z = sorted_half(1)
            split[sp, 64:256] = z[32:224]
            rows_of = {2: [split[sp, 0:32], split[sp, 32:64], z[0:32]]}
        else:
            rows_of = {u: [split[sp, 96 * u - 224 + 32 * t : 96 * u - 192 + 32 * t] for t in range(3)] for u in cycles}
        for u, tiles in rows_of.items():
            pieces = []
            for h in range(2):
                zu = jnp.concatenate([x[:, h * 128 : h * 128 + 128] for x in tiles], axis=1)
                pieces += [zu * sections[m] for m in range(4)]
            y = nt_dot(spread[...], jnp.concatenate(pieces, axis=0))
            for h in range(2):
                part = (y[:, h * 128 : h * 128 + 128] * factor).astype(BF)
                for r in range(2):
                    for f in range(3):
                        rows = pl.ds(pl.multiple_of(f * 128 + sp * 32 + h * 16, 16), 16)
                        fields[u, rows, r * 128 : r * 128 + 128] = part[r * 48 + f * 16 : r * 48 + f * 16 + 16, :]
        return 0

    lax.fori_loop(0, 4, pair, 0, unroll=2)


def grid_cycle(u, points, coef_row, table, fields, tend, analysed):
    for a in range(10):
        cols = slice(a * 256, a * 256 + 256)
        g = nn_dot(fields[u], table[u, :, cols])
        coef = coef_row[:, cols]
        for f in range(3):
            nxt = (f + 1) % 3
            tend[f * 128 : f * 128 + 128, cols] = (
                g[f * 128 : f * 128 + 128] * (coef + g[nxt * 128 : nxt * 128 + 128])
            ).astype(BF)
    total = nt_dot(table[u], tend[...])
    share = 1.0 / jnp.full((1, 384), points, jnp.int32).astype(F32)
    analysed[u] = (total * share).astype(BF)


def pack_return(half, back, analysed, send):
    places = [divmod(half * 8 + i, 3) for i in range(8)]

    def pair(g, _):
        groups = []
        for h in range(2):
            rows = pl.ds(pl.multiple_of(g * 64 + h * 32, 32), 32)
            groups.append(
                jnp.concatenate(
                    [
                        analysed[u, rows, f * 128 : f * 128 + 128] if u < CYC else jnp.zeros((32, 128), BF)
                        for u, f in places
                    ],
                    axis=0,
                )
            )
        y = nn_dot(back[...], jnp.concatenate(groups, axis=1)).astype(BF)
        for h in range(2):
            rows = pl.ds(pl.multiple_of(half * HALF + g * 512 + h * 256, 256), 256)
            send[rows, :] = y[:, h * 128 : h * 128 + 128]
        return 0

    lax.fori_loop(0, 4, pair, 0, unroll=2)


def parity_parts(recv, packt, weight_col, parts):
    def block(g, _):
        rows = pl.ds(pl.multiple_of(g * 80, 16), 80)
        sides = []
        for side in range(2):
            starts = [pl.multiple_of(half * HALF + side * 1024 + g * 128, 128) for half in range(2)]
            sides.append(jnp.concatenate([recv[pl.ds(x, 128), :] for x in starts], axis=0))
        x = jnp.concatenate(sides, axis=1)
        z = nn_dot(packt[...], x)
        weight = weight_col[rows, :]
        for f in range(3):
            north = z[f * 80 : f * 80 + 80, :128]
            south = z[f * 80 : f * 80 + 80, 128:]
            parts[f, rows, 0:128] = (weight * (north + south)).astype(BF)
            parts[f, rows, 128:256] = (weight * (north - south)).astype(BF)
        return 0

    lax.fori_loop(0, 8, block, 0, unroll=4)


def make_damp(wave, depth_col, damp):
    for a in range(NT // 128):
        degree = (lax.broadcasted_iota(jnp.int32, (1, 128), 1) + (wave + a * 128)).astype(F32)
        damp[:, a * 128 : a * 128 + 128] = 1.0 / (1.0 + depth_col[...] * degree * (degree + 1.0) / float(NT * NT))


def forward_modes(leg_m, length, eye, parts, flipped, modes_in, modes_out, damp, update, ready):
    for f in range(3):
        t = nt_dot(eye[...], parts[f]).astype(BF)
        flipped[f * 128 : f * 128 + 128, :] = t[:128]
        flipped[384 + f * 128 : 512 + f * 128, :] = t[128:]
    lane = lax.broadcasted_iota(jnp.int32, (1, 256), 1)
    even_lane = lane % 2 == 0

    def block(ic, _):
        cols = pl.ds(pl.multiple_of(ic * 256, 256), 256)
        both = nn_dot(flipped[...], leg_m(cols))
        live = lane + ic * 256 < length
        for f in range(3):
            even = both[f * 128 : f * 128 + 128]
            odd = both[384 + f * 128 : 512 + f * 128]
            proj = jnp.where(live, jnp.where(even_lane, even, odd), 0.0).astype(BF)
            scaled = (nn_dot(modes_in[...], proj) * damp[:, cols]).astype(BF)
            update[f, :, cols] = nn_dot(modes_out[...], scaled).astype(BF)
        ready(ic)
        return 0

    lax.fori_loop(0, NT // 256, block, 0)


def column_of(row):
    return jnp.transpose(jnp.broadcast_to(row, (128, 128)))


def side_columns(waves_row, weights, depths_row, wave_col, wave_row, weight_col, depth_col):
    place = lax.broadcasted_iota(jnp.int32, (128, 128), 0)
    slot = lax.broadcasted_iota(jnp.int32, (128, 128), 1)
    order = jnp.where((place % 32) * 4 + place // 32 == slot, 1.0, 0.0).astype(BF)
    rows = jnp.broadcast_to(waves_row[...], (128, 128))
    high = (rows // 32).astype(F32).astype(BF)
    low = (rows % 32).astype(F32).astype(BF)
    column = nt_dot(order, high) * 32.0 + nt_dot(order, low)
    wave_col[...] = column
    wave_row[...] = jnp.transpose(column)[0:8]
    for i in range(5):
        weight_col[i * 128 : i * 128 + 128, :] = column_of(weights[i : i + 1, :])
    depth_col[...] = column_of(depths_row[...])


def send_half(half, send, recv, sems, source_slot, my_slot):
    w, s = position()

    def rows(slot):
        return pl.ds(pl.multiple_of(half * HALF + slot * 8, 8), 8)

    pltpu.make_async_copy(send.at[rows(source_slot(w, s))], recv.at[rows(my_slot)], sems.at[half, 0]).start()

    def start(i, _):
        tw = lax.rem(w + lax.rem(i, WAVES), WAVES)
        ts = lax.rem(s + i // WAVES, LEVS)
        pltpu.make_async_remote_copy(
            src_ref=send.at[rows(source_slot(tw, ts))],
            dst_ref=recv.at[rows(my_slot)],
            send_sem=sems.at[half, 1],
            recv_sem=sems.at[half, 2],
            device_id=(tw, ts),
            device_id_type=MESH,
        ).start()
        return 0

    lax.fori_loop(1, DEVS, start, 0)


def wait_half(half, send, recv, sems):
    rest = pl.ds(half * HALF, HALF - 8)
    block = pl.ds(half * HALF, 8)
    pltpu.make_async_copy(send.at[block], recv.at[block], sems.at[half, 0]).wait()
    pltpu.make_async_copy(recv.at[rest], recv.at[rest], sems.at[half, 2]).wait()


def wait_sent(half, send, sems):
    rest = pl.ds(half * HALF, HALF - 8)
    pltpu.make_async_copy(send.at[rest], send.at[rest], sems.at[half, 1]).wait()


def signal_peers(sem, peers):
    for peer in peers:
        pl.semaphore_signal(sem, inc=1, device_id=shifted(*peer), device_id_type=MESH)


PLANE_PEERS = [(0, dy, dx, dc) for dx in range(4) for dy in range(4) for dc in range(2) if dx or dy or dc]
Z_PEERS = [(dz, 0, 0, 0) for dz in range(1, 8)]
N_LATE = 17


def whole(
    lens_hbm,
    waves_hbm,
    cyc_hbm,
    spec_hbm,
    leg_hbm,
    pack_hbm,
    coef_hbm,
    unpack_hbm,
    spread_hbm,
    back_hbm,
    packt_hbm,
    eye_hbm,
    weights_hbm,
    waves_row_hbm,
    depths_row_hbm,
    modes_in_hbm,
    modes_out_hbm,
    out,
    lens,
    waves,
    cyc,
    waves_row,
    depths_row,
    modes_in,
    modes_out,
    damp,
    spec,
    leg,
    pack,
    coef,
    unpack,
    spread,
    back,
    packt,
    eye,
    rhs,
    waves_out,
    send_a,
    recv_a,
    split,
    table,
    low,
    fields,
    tend,
    analysed,
    send_b,
    recv_b,
    parts,
    flipped,
    update,
    wave_col,
    wave_row,
    weight_col,
    depth_col,
    weights,
    load_sem,
    late_sem,
    z_sem,
    sems_a,
    sems_b,
    sems_c,
):
    w, s = position()
    dest = w * LEVS + s
    m, r = s // 2, lax.rem(s, 2)
    barrier = pltpu.get_barrier_semaphore()

    loads = [pltpu.make_async_copy(spec_hbm, spec, load_sem.at[0])]
    loads += [pltpu.make_async_copy(leg_hbm.at[i], leg.at[i], load_sem.at[1 + i]) for i in range(4)]
    loads += [pltpu.make_async_copy(pack_hbm, pack, load_sem.at[5]), pltpu.make_async_copy(lens_hbm, lens, load_sem.at[6])]
    late = [
        pltpu.make_async_copy(a, b, late_sem.at[i])
        for i, (a, b) in enumerate(
            [
                (coef_hbm, coef),
                (unpack_hbm, unpack),
                (spread_hbm, spread),
                (back_hbm, back),
                (packt_hbm, packt),
                (eye_hbm, eye),
                (waves_hbm, waves),
                (cyc_hbm, cyc),
                (waves_row_hbm, waves_row),
                (depths_row_hbm, depths_row),
                (modes_in_hbm, modes_in),
                (modes_out_hbm, modes_out),
                *[(weights_hbm.at[pl.ds(i * 128, 128)], weights.at[i]) for i in range(5)],
            ]
        )
    ]
    for copy in [loads[6]] + loads[:6] + late:
        copy.start()

    signal_peers(barrier, Z_PEERS + PLANE_PEERS)
    loads[6].wait()
    loads[0].wait()
    inverse_rows(spec, lambda i: lens[w * 4 + i], rhs)
    loads[1].wait()
    loads[2].wait()
    inverse_dots(0, leg, rhs, waves_out)
    pl.semaphore_wait(barrier, len(Z_PEERS + PLANE_PEERS))
    signal_peers(z_sem, Z_PEERS)
    loads[3].wait()
    inverse_dots(1, leg, rhs, waves_out)
    loads[4].wait()
    inverse_dots(2, leg, rhs, waves_out)
    loads[5].wait()
    inverse_pack(pack, waves_out, send_a)
    pl.semaphore_wait(z_sem, len(Z_PEERS))

    for half in range(2):
        send_half(half, send_a, recv_a, sems_a, lambda tw, ts: mirrored(tw * LEVS + ts), s * WAVES + w)

    for copy in late:
        copy.wait()
    side_columns(waves_row, weights, depths_row, wave_col, wave_row, weight_col, depth_col)

    def shift(u):
        return jnp.where(dest < 128, u, 4 - u)

    def make_table(u, _):
        cycle_table(u, wave_col, cyc[dest * CYC + shift(u)], table, low)
        return 0

    lax.fori_loop(0, CYC, make_table, 0)

    def cycle(u, _):
        points = cyc[dest * CYC + shift(u)]
        grid_cycle(u, points, coef[pl.ds(s * CYC + shift(u), 1), :], table, fields, tend, analysed)
        return 0

    def return_half(half):
        pack_return(half, back, analysed, send_b)
        send_half(
            half,
            send_b,
            recv_b,
            sems_b,
            lambda tw, ts: lax.rem(ts, 2) * 128 + (ts // 2) * 32 + tw,
            mirrored(w * LEVS + s),
        )

    wait_half(0, send_a, recv_a, sems_a)
    gather_waves((0, 1), recv_a, unpack, spread, wave_row, split, fields)
    lax.fori_loop(0, 2, cycle, 0)
    wait_half(1, send_a, recv_a, sems_a)
    gather_waves((2,), recv_a, unpack, spread, wave_row, split, fields)
    cycle(2, 0)
    return_half(0)
    gather_waves((3, 4), recv_a, unpack, spread, wave_row, split, fields)
    lax.fori_loop(3, CYC, cycle, 0)
    return_half(1)
    make_damp(waves[w * 4 + m], depth_col, damp)
    for half in range(2):
        wait_sent(half, send_a, sems_a)
        wait_half(half, send_b, recv_b, sems_b)
        wait_sent(half, send_b, sems_b)

    def to_levels(ic):
        cols = pl.ds(pl.multiple_of(ic * 256, 256), 256)
        place = out.at[m, pl.ds(r * 3, 3), :, cols]

        def piece(ts):
            return update.at[:, pl.ds(pl.multiple_of(ts * 16, 16), 16), cols]

        for i in range(1, LEVS):
            ts = lax.rem(s + i, LEVS)
            pltpu.make_async_remote_copy(
                src_ref=piece(ts),
                dst_ref=place,
                send_sem=sems_c.at[0],
                recv_sem=sems_c.at[1],
                device_id=(w, ts),
                device_id_type=MESH,
            ).start()
        pltpu.make_async_copy(piece(s), place, sems_c.at[1]).start()

    parity_parts(recv_b, packt, weight_col, parts)
    forward_modes(
        lambda cols: leg[m, :, cols],
        lens[w * 4 + m],
        eye,
        parts,
        flipped,
        modes_in,
        modes_out,
        damp,
        update,
        to_levels,
    )
    sent = update.at[:, 0:112, :]
    pltpu.make_async_copy(sent, sent, sems_c.at[0]).wait()
    pltpu.make_async_copy(out, out, sems_c.at[1]).wait()


VM = pl.BlockSpec(memory_space=pltpu.VMEM)
SM = pl.BlockSpec(memory_space=pltpu.SMEM)
ANY = pl.BlockSpec(memory_space=pl.ANY)


def on_device(
    spectral,
    legendre,
    wave_ids,
    trunc_lengths,
    cycle_points,
    grid_coef,
    cycle_weights,
    modes_in,
    modes_out,
    depths,
):
    pack, unpack, spread, back, packt, eye = [jnp.asarray(x, BF) for x in constant_arrays()]
    vmem = pltpu.VMEM
    return pl.pallas_call(
        whole,
        out_shape=pltpu.VMEM((4, 6, 16, NT), BF),
        in_specs=[ANY] * 17,
        out_specs=VM,
        scratch_shapes=[
            pltpu.SMEM((128,), jnp.int32),
            pltpu.SMEM((128,), jnp.int32),
            pltpu.SMEM((NT,), jnp.int32),
            vmem((1, 128), jnp.int32),
            vmem((1, 128), F32),
            vmem((128, 128), BF),
            vmem((128, 128), BF),
            vmem((128, NT), F32),
            vmem((384, NT), BF),
            vmem((4, 640, NT), BF),
            vmem((256, 240), BF),
            vmem((40, 2560), F32),
            vmem((256, 256), BF),
            vmem((96, 384), BF),
            vmem((256, 256), BF),
            vmem((240, 256), BF),
            vmem((256, 256), BF),
            vmem((6, 256, NT), BF),
            vmem((3, 640, 256), BF),
            vmem((2 * HALF, 128), BF),
            vmem((2 * HALF, 128), BF),
            vmem((4, 256, 256), BF),
            vmem((CYC, 256, 2560), BF),
            vmem((2, 128, 256), F32),
            vmem((CYC, 384, 256), BF),
            vmem((384, 2560), BF),
            vmem((CYC, 256, 384), BF),
            vmem((2 * HALF, 128), BF),
            vmem((2 * HALF, 128), BF),
            vmem((3, 640, 256), BF),
            vmem((768, 640), BF),
            vmem((3, 128, NT), BF),
            vmem((128, 128), F32),
            vmem((8, 128), F32),
            vmem((640, 128), F32),
            vmem((128, 128), F32),
            vmem((8, 128), F32),
            pltpu.SemaphoreType.DMA((7,)),
            pltpu.SemaphoreType.DMA((N_LATE,)),
            pltpu.SemaphoreType.REGULAR,
            pltpu.SemaphoreType.DMA((2, 3)),
            pltpu.SemaphoreType.DMA((2, 3)),
            pltpu.SemaphoreType.DMA((2,)),
        ],
        name="whole",
        compiler_params=pltpu.CompilerParams(
            vmem_limit_bytes=56 * 1024 * 1024, collective_id=0, has_side_effects=True
        ),
    )(
        trunc_lengths,
        wave_ids,
        cycle_points,
        spectral.reshape(384, NT),
        legendre,
        pack,
        grid_coef,
        unpack,
        spread,
        back,
        packt,
        eye,
        cycle_weights,
        wave_ids.reshape(1, 128),
        depths.reshape(1, 128),
        modes_in,
        modes_out,
    )


def solution(mesh):
    placed = (
        P("wave", None, "lev", None),
        P("wave", None, None),
        P(),
        P(),
        P(),
        P("wave", None),
        P(),
        P(),
        P(),
        P(),
    )
    return jax.shard_map(
        on_device,
        mesh=mesh,
        in_specs=placed,
        out_specs=P("wave", None, "lev", None),
        check_vma=False,
    )
```

```python
import jax
import jax.numpy as jnp
import numpy as np
from jax import lax
from jax.experimental import pallas as pl
from jax.experimental.pallas import tpu as pltpu
from jax.sharding import PartitionSpec as P

MESH = pl.DeviceIdType.MESH
NT = 1280
BF = jnp.bfloat16
F32 = jnp.float32
WAVES = 32
LEVS = 8
DEVS = 256
CYC = 5
UNROLL = 4
CHUNKS = ((0, 256), (256, 256), (512, 256), (768, 256), (1024, 256))
HALF = DEVS * 8
SECTIONS = ((0, 0, 0, 96), (0, 1, 96, 128), (1, 1, 0, 64), (1, 2, 64, 128), (2, 2, 0, 32), (2, 3, 32, 128))


def nt_dot(a, b):
    return lax.dot_general(a, b, (((1,), (1,)), ((), ())), preferred_element_type=F32)


def nn_dot(a, b):
    return lax.dot_general(a, b, (((1,), (0,)), ((), ())), preferred_element_type=F32)


def constant_arrays():
    half, rest = np.divmod(np.arange(256), 128)
    block, row = np.divmod(rest, 8)
    row = row + half * 8
    tile, cyc = np.divmod(np.arange(240), 80)
    pack = (row[:, None] < 15) & (row[:, None] % 3 == tile[None]) & (5 * block[:, None] + row[:, None] // 3 == cyc[None])
    out_row, out_w = np.divmod(np.arange(256), 32)
    in_w, in_row = np.divmod(np.arange(256), 8)
    unpack = (out_w[:, None] == in_w[None]) & (out_row[:, None] == in_row[None])
    spread = np.arange(96)[:, None] == np.arange(384)[None] % 96
    return [x.astype(np.float32) for x in (pack, unpack, spread, unpack.T, pack.T, np.eye(256))]


def position():
    return lax.axis_index("wave"), lax.axis_index("lev")


def shifted(dz, dy, dx, dc):
    w, s = position()
    tw = lax.rem(w // 4 + dz, 8) * 4 + lax.rem(w + dy, 4)
    return tw, lax.rem(s // 2 + dx, 4) * 2 + lax.rem(s + dc, 2)


def mirrored(dest):
    return jnp.where(dest < 128, dest, 383 - dest)


def inverse_rows(spec_ref, len_of, rhs):
    column = lax.broadcasted_iota(jnp.int32, (1, NT), 1)
    for idx, (t, m, lo, hi) in enumerate(SECTIONS):
        live = column < len_of(m)
        north = jnp.where(live, 1.0, 0.0).astype(BF)
        south = jnp.where(live, jnp.where(column % 2 == 0, 1.0, -1.0), 0.0).astype(BF)
        for half, factor in ((0, north), (128, south)):
            if lo > 0:
                rhs[idx, half : half + lo, :] = jnp.zeros((lo, NT), BF)
            if hi < 128:
                rhs[idx, half + hi : half + 128, :] = jnp.zeros((128 - hi, NT), BF)
            rhs[idx, half + lo : half + hi, :] = spec_ref[t * 128 + lo : t * 128 + hi, :] * factor


def inverse_dots(t, leg, rhs, waves_out):
    step = 320
    ma, mb = SECTIONS[2 * t][1], SECTIONS[2 * t + 1][1]

    def block(jc, _):
        rows = pl.ds(pl.multiple_of(jc * step, 64), step)
        out = nt_dot(leg[ma, rows, :], rhs[2 * t]) + nt_dot(leg[mb, rows, :], rhs[2 * t + 1])
        waves_out[t, rows, :] = out.astype(BF)
        return 0

    lax.fori_loop(0, 640 // step, block, 0)


def inverse_pack(pack, waves_out, send):
    def block(g, _):
        rows = pl.ds(pl.multiple_of(g * 80, 16), 80)
        x = jnp.concatenate([waves_out[t, rows, :] for t in range(3)], axis=0)
        y = nn_dot(pack[...], x).astype(BF)
        for half in range(2):
            for side in range(2):
                rows = pl.ds(pl.multiple_of(half * HALF + side * 1024 + g * 128, 128), 128)
                send[rows, :] = y[half * 128 : half * 128 + 128, side * 128 : side * 128 + 128]
        return 0

    lax.fori_loop(0, 8, block, 0, unroll=4)


def cos_sin(steps, count):
    turns = jnp.round(steps * (4.0 / count))
    rest = steps - turns * (count * 0.25)
    x = rest * (2.0 * np.pi / count)
    x2 = x * x
    sine = x * (1.0 + x2 * (-1.0 / 6 + x2 * (1.0 / 120 + x2 * (-1.0 / 5040 + x2 * (1.0 / 362880)))))
    cosine = 1.0 + x2 * (-0.5 + x2 * (1.0 / 24 + x2 * (-1.0 / 720 + x2 * (1.0 / 40320))))
    quadrant = turns.astype(jnp.int32) & 3
    swap = (quadrant & 1) == 1
    c = jnp.where(swap, sine, cosine)
    s = jnp.where(swap, cosine, sine)
    c = jnp.where((quadrant == 1) | (quadrant == 2), -c, c)
    s = jnp.where(quadrant >= 2, -s, s)
    return c, s


def cycle_table(u, wave_col, points, table, low):
    count = jnp.full((1, 128), points, jnp.int32).astype(F32)
    lane = lax.broadcasted_iota(jnp.int32, (1, 128), 1)
    lane_f = lane.astype(F32)
    waves = wave_col[...]
    for half in range(2):
        c, s = cos_sin(waves * (lane_f + 128.0 * half), count)
        low[0, :, half * 128 : half * 128 + 128] = c
        low[1, :, half * 128 : half * 128 + 128] = s
    c_high, s_high = cos_sin(waves * (lane_f * 256.0), count)
    live = 2.0 * waves < count
    c_high = jnp.where(live, c_high, 0.0)
    s_high = jnp.where(live, s_high, 0.0)
    wide = lax.broadcasted_iota(jnp.int32, (1, 256), 1)
    for a in range(10):
        ca = c_high[:, a : a + 1]
        sa = s_high[:, a : a + 1]
        keep = jnp.where(wide + 256 * a < points, 1.0, 0.0)
        cl = low[0] * keep
        sl = low[1] * keep
        cols = slice(a * 256, a * 256 + 256)
        table[u, 0:128, cols] = (cl * ca - sl * sa).astype(BF)
        table[u, 128:256, cols] = (-(sl * ca + cl * sa)).astype(BF)


def gather_waves(cycles, recv, unpack, spread, wave_row, split, fields):
    lane = lax.broadcasted_iota(jnp.int32, (1, 384), 1)
    sections = [jnp.where((lane >= 96 * m) & (lane < 96 * m + 96), 1.0, 0.0).astype(BF) for m in range(4)]
    factor = jnp.where(wave_row[0:1, :] == 0.0, 1.0, 2.0)

    def pair(sp, _):
        def sorted_half(half):
            starts = [pl.multiple_of(half * HALF + sp * 512 + h * 256, 256) for h in range(2)]
            return nn_dot(unpack[...], jnp.concatenate([recv[pl.ds(x, 256), :] for x in starts], axis=1)).astype(BF)

        if cycles == (0, 1):
            z = sorted_half(0)
            split[sp, 0:64] = z[192:256]
            rows_of = {u: [z[96 * u + 32 * t : 96 * u + 32 * t + 32] for t in range(3)] for u in cycles}
        elif cycles == (2,):
            z = sorted_half(1)
            split[sp, 64:256] = z[32:224]
            rows_of = {2: [split[sp, 0:32], split[sp, 32:64], z[0:32]]}
        else:
            rows_of = {u: [split[sp, 96 * u - 224 + 32 * t : 96 * u - 192 + 32 * t] for t in range(3)] for u in cycles}
        for u, tiles in rows_of.items():
            pieces = []
            for h in range(2):
                zu = jnp.concatenate([x[:, h * 128 : h * 128 + 128] for x in tiles], axis=1)
                pieces += [zu * sections[m] for m in range(4)]
            y = nt_dot(spread[...], jnp.concatenate(pieces, axis=0))
            for h in range(2):
                part = (y[:, h * 128 : h * 128 + 128] * factor).astype(BF)
                for r in range(2):
                    for f in range(3):
                        rows = pl.ds(pl.multiple_of(f * 128 + sp * 32 + h * 16, 16), 16)
                        fields[u, rows, r * 128 : r * 128 + 128] = part[r * 48 + f * 16 : r * 48 + f * 16 + 16, :]
        return 0

    lax.fori_loop(0, 4, pair, 0, unroll=2)


def grid_cycle(u, points, coef_row, table, fields, tend, analysed):
    for a in range(10):
        cols = slice(a * 256, a * 256 + 256)
        g = nn_dot(fields[u], table[u, :, cols])
        coef = coef_row[:, cols]
        for f in range(3):
            nxt = (f + 1) % 3
            tend[f * 128 : f * 128 + 128, cols] = (
                g[f * 128 : f * 128 + 128] * (coef + g[nxt * 128 : nxt * 128 + 128])
            ).astype(BF)
    total = nt_dot(table[u], tend[...])
    share = 1.0 / jnp.full((1, 384), points, jnp.int32).astype(F32)
    analysed[u] = (total * share).astype(BF)


def pack_return(half, back, analysed, send):
    places = [divmod(half * 8 + i, 3) for i in range(8)]

    def pair(g, _):
        groups = []
        for h in range(2):
            rows = pl.ds(pl.multiple_of(g * 64 + h * 32, 32), 32)
            groups.append(
                jnp.concatenate(
                    [
                        analysed[u, rows, f * 128 : f * 128 + 128] if u < CYC else jnp.zeros((32, 128), BF)
                        for u, f in places
                    ],
                    axis=0,
                )
            )
        y = nn_dot(back[...], jnp.concatenate(groups, axis=1)).astype(BF)
        for h in range(2):
            rows = pl.ds(pl.multiple_of(half * HALF + g * 512 + h * 256, 256), 256)
            send[rows, :] = y[:, h * 128 : h * 128 + 128]
        return 0

    lax.fori_loop(0, 4, pair, 0, unroll=2)


def parity_parts(recv, packt, weight_col, parts):
    def block(g, _):
        rows = pl.ds(pl.multiple_of(g * 80, 16), 80)
        sides = []
        for side in range(2):
            starts = [pl.multiple_of(half * HALF + side * 1024 + g * 128, 128) for half in range(2)]
            sides.append(jnp.concatenate([recv[pl.ds(x, 128), :] for x in starts], axis=0))
        x = jnp.concatenate(sides, axis=1)
        z = nn_dot(packt[...], x)
        weight = weight_col[rows, :]
        for f in range(3):
            north = z[f * 80 : f * 80 + 80, :128]
            south = z[f * 80 : f * 80 + 80, 128:]
            parts[f, rows, 0:128] = (weight * (north + south)).astype(BF)
            parts[f, rows, 128:256] = (weight * (north - south)).astype(BF)
        return 0

    lax.fori_loop(0, 8, block, 0, unroll=4)


def make_damp(wave, depth_col, damp):
    for a in range(NT // 128):
        degree = (lax.broadcasted_iota(jnp.int32, (1, 128), 1) + (wave + a * 128)).astype(F32)
        damp[:, a * 128 : a * 128 + 128] = 1.0 / (1.0 + depth_col[...] * degree * (degree + 1.0) / float(NT * NT))


def forward_modes(leg_m, length, eye, parts, flipped, modes_in, modes_out, damp, update, ready):
    for f in range(3):
        t = nt_dot(eye[...], parts[f]).astype(BF)
        flipped[f * 128 : f * 128 + 128, :] = t[:128]
        flipped[384 + f * 128 : 512 + f * 128, :] = t[128:]
    lane = lax.broadcasted_iota(jnp.int32, (1, 256), 1)
    even_lane = lane % 2 == 0

    def project(start, width):
        both = nn_dot(flipped[...], leg_m(slice(start, start + width)))
        live = lane[:, :width] + start < length
        parts = []
        for f in range(3):
            even = both[f * 128 : f * 128 + 128]
            odd = both[384 + f * 128 : 512 + f * 128]
            parts.append(jnp.where(live, jnp.where(even_lane[:, :width], even, odd), 0.0).astype(BF))
        return jnp.concatenate(parts, axis=1)

    def mix(start, width, proj):
        cols = slice(start, start + width)
        vals = nn_dot(modes_in[...], proj)
        scaled = (vals * jnp.concatenate([damp[:, cols]] * 3, axis=1)).astype(BF)
        mixed = nn_dot(modes_out[...], scaled).astype(BF)
        for f in range(3):
            update[f, :, cols] = mixed[:, f * width : f * width + width]

    proj = project(*CHUNKS[0])
    for chunk, following in zip(CHUNKS, CHUNKS[1:] + (None,)):
        after = project(*following) if following else None
        mix(*chunk, proj)
        ready(*chunk)
        proj = after


def column_of(row):
    return jnp.transpose(jnp.broadcast_to(row, (128, 128)))


def side_columns(waves_row, weights, depths_row, wave_col, wave_row, weight_col, depth_col):
    place = lax.broadcasted_iota(jnp.int32, (128, 128), 0)
    slot = lax.broadcasted_iota(jnp.int32, (128, 128), 1)
    order = jnp.where((place % 32) * 4 + place // 32 == slot, 1.0, 0.0).astype(BF)
    rows = jnp.broadcast_to(waves_row[...], (128, 128))
    high = (rows // 32).astype(F32).astype(BF)
    low = (rows % 32).astype(F32).astype(BF)
    column = nt_dot(order, high) * 32.0 + nt_dot(order, low)
    wave_col[...] = column
    wave_row[...] = jnp.transpose(column)[0:8]
    for i in range(5):
        weight_col[i * 128 : i * 128 + 128, :] = column_of(weights[i : i + 1, :])
    depth_col[...] = column_of(depths_row[...])


def send_class(half, core, send, recv, spare, sems, source_slot, my_slot):
    w, s = position()

    def rows(slot):
        return pl.ds(pl.multiple_of(half * HALF + slot * 8, 8), 8)

    def start(tw, ts):
        pltpu.make_async_remote_copy(
            src_ref=send.at[rows(source_slot(tw, ts))],
            dst_ref=recv.at[rows(my_slot)],
            send_sem=sems.at[half, core],
            recv_sem=sems.at[half, 2],
            device_id=(tw, ts),
            device_id_type=MESH,
        ).start()

    for k in range(LEVS // 2):
        ts = ((s // 2 + k) & 3) * 2 + core
        if k == 0:
            own = (s & 1) == core
            pl.when(jnp.logical_not(own))(lambda ts=ts: start(w, ts))

            @pl.when(own)
            def _():
                source = send.at[rows(source_slot(w, s))]
                pltpu.make_async_copy(source, recv.at[rows(my_slot)], sems.at[half, 3]).start()
                pltpu.make_async_copy(source, spare.at[half], sems.at[half, core]).start()

        else:
            start(w, ts)
        lax.fori_loop(1, WAVES, lambda i, c, ts=ts: (start((w + i) & 31, ts), c)[1], 0, unroll=UNROLL)


def wait_sent(half, core, send, sems):
    part = send.at[pl.ds(half * HALF, HALF // 2)]
    pltpu.make_async_copy(part, part, sems.at[half, core]).wait()


def wait_half(half, recv, sems):
    rest = recv.at[pl.ds(half * HALF, HALF - 8)]
    own = recv.at[pl.ds(half * HALF, 8)]
    pltpu.make_async_copy(own, own, sems.at[half, 3]).wait()
    pltpu.make_async_copy(rest, rest, sems.at[half, 2]).wait()


def signal_peers(sem, peers):
    for peer in peers:
        pl.semaphore_signal(sem, inc=1, device_id=shifted(*peer), device_id_type=MESH)


PLANE_PEERS = [(0, dy, dx, dc) for dx in range(4) for dy in range(4) for dc in range(2) if dx or dy or dc]
Z_PEERS = [(dz, 0, 0, 0) for dz in range(1, 8)]
N_LATE = 17


def whole(
    lens_hbm,
    waves_hbm,
    cyc_hbm,
    spec_hbm,
    leg_hbm,
    pack_hbm,
    coef_hbm,
    unpack_hbm,
    spread_hbm,
    back_hbm,
    packt_hbm,
    eye_hbm,
    weights_hbm,
    waves_row_hbm,
    depths_row_hbm,
    modes_in_hbm,
    modes_out_hbm,
    out,
    lens,
    waves,
    cyc,
    waves_row,
    depths_row,
    modes_in,
    modes_out,
    damp,
    spec,
    leg,
    pack,
    coef,
    unpack,
    spread,
    back,
    packt,
    eye,
    rhs,
    waves_out,
    send_a,
    recv_a,
    split,
    table,
    low,
    fields,
    tend,
    analysed,
    send_b,
    recv_b,
    parts,
    flipped,
    update,
    wave_col,
    wave_row,
    weight_col,
    depth_col,
    weights,
    spare_a,
    spare_b,
    load_sem,
    late_sem,
    z_sem,
    sems_a,
    sems_b,
    sems_c,
):
    w, s = position()
    dest = w * LEVS + s
    m, r = s // 2, lax.rem(s, 2)
    barrier = pltpu.get_barrier_semaphore()

    loads = [pltpu.make_async_copy(spec_hbm, spec, load_sem.at[0])]
    loads += [pltpu.make_async_copy(leg_hbm.at[i], leg.at[i], load_sem.at[1 + i]) for i in range(4)]
    loads += [pltpu.make_async_copy(pack_hbm, pack, load_sem.at[5]), pltpu.make_async_copy(lens_hbm, lens, load_sem.at[6])]
    late = [
        pltpu.make_async_copy(a, b, late_sem.at[i])
        for i, (a, b) in enumerate(
            [
                (coef_hbm, coef),
                (unpack_hbm, unpack),
                (spread_hbm, spread),
                (back_hbm, back),
                (packt_hbm, packt),
                (eye_hbm, eye),
                (waves_hbm, waves),
                (cyc_hbm, cyc),
                (waves_row_hbm, waves_row),
                (depths_row_hbm, depths_row),
                (modes_in_hbm, modes_in),
                (modes_out_hbm, modes_out),
                *[(weights_hbm.at[pl.ds(i * 128, 128)], weights.at[i]) for i in range(5)],
            ]
        )
    ]
    for copy in [loads[6]] + loads[:6] + late:
        copy.start()

    signal_peers(barrier, Z_PEERS + PLANE_PEERS)
    loads[6].wait()
    loads[0].wait()
    inverse_rows(spec, lambda i: lens[w * 4 + i], rhs)
    loads[1].wait()
    loads[2].wait()
    inverse_dots(0, leg, rhs, waves_out)
    pl.semaphore_wait(barrier, len(Z_PEERS + PLANE_PEERS))
    signal_peers(z_sem, Z_PEERS)
    loads[3].wait()
    inverse_dots(1, leg, rhs, waves_out)
    loads[4].wait()
    inverse_dots(2, leg, rhs, waves_out)
    loads[5].wait()
    inverse_pack(pack, waves_out, send_a)
    pl.semaphore_wait(z_sem, len(Z_PEERS))

    def to_cycles(half, core):
        send_class(half, core, send_a, recv_a, spare_a, sems_a, lambda tw, ts: mirrored(tw * LEVS + ts), s * WAVES + w)

    def to_waves(half, core):
        send_class(
            half,
            core,
            send_b,
            recv_b,
            spare_b,
            sems_b,
            lambda tw, ts: ((ts & 1) * 4 + (ts >> 1)) * 32 + tw,
            mirrored(w * LEVS + s),
        )

    def shift(u):
        return jnp.where(dest < 128, u, 4 - u)

    def make_table(u, _):
        cycle_table(u, wave_col, cyc[dest * CYC + shift(u)], table, low)
        return 0

    to_cycles(0, 0)
    for copy in late:
        copy.wait()
    side_columns(waves_row, weights, depths_row, wave_col, wave_row, weight_col, depth_col)
    make_table(0, 0)
    to_cycles(1, 0)
    lax.fori_loop(1, CYC, make_table, 0)
    wait_sent(0, 0, send_a, sems_a)
    to_cycles(0, 1)
    to_cycles(1, 1)

    def cycle(u, _):
        points = cyc[dest * CYC + shift(u)]
        grid_cycle(u, points, coef[pl.ds(s * CYC + shift(u), 1), :], table, fields, tend, analysed)
        return 0

    wait_half(0, recv_a, sems_a)
    gather_waves((0, 1), recv_a, unpack, spread, wave_row, split, fields)
    lax.fori_loop(0, 2, cycle, 0)
    wait_half(1, recv_a, sems_a)
    gather_waves((2,), recv_a, unpack, spread, wave_row, split, fields)
    cycle(2, 0)
    pack_return(0, back, analysed, send_b)
    to_waves(0, 0)
    gather_waves((3, 4), recv_a, unpack, spread, wave_row, split, fields)
    pl.when((s & 1) == 0)(lambda: to_waves(0, 1))
    lax.fori_loop(3, CYC, cycle, 0)
    pack_return(1, back, analysed, send_b)
    to_waves(1, 0)
    pl.when((s & 1) == 1)(lambda: to_waves(0, 1))
    make_damp(waves[w * 4 + m], depth_col, damp)
    to_waves(1, 1)
    for half in range(2):
        wait_half(half, recv_b, sems_b)

    def to_levels(start, width):
        cols = pl.ds(start, width)
        place = out.at[m, pl.ds(r * 3, 3), :, cols]

        def piece(ts):
            return update.at[:, pl.ds(pl.multiple_of(ts * 16, 16), 16), cols]

        for i in range(1, LEVS):
            ts = lax.rem(s + i, LEVS)
            pltpu.make_async_remote_copy(
                src_ref=piece(ts),
                dst_ref=place,
                send_sem=sems_c.at[0],
                recv_sem=sems_c.at[1],
                device_id=(w, ts),
                device_id_type=MESH,
            ).start()
        pltpu.make_async_copy(piece(s), place, sems_c.at[1]).start()

    parity_parts(recv_b, packt, weight_col, parts)
    forward_modes(
        lambda cols: leg[m, :, cols],
        lens[w * 4 + m],
        eye,
        parts,
        flipped,
        modes_in,
        modes_out,
        damp,
        update,
        to_levels,
    )
    for half in range(2):
        wait_sent(half, 1, send_a, sems_a)
        if half == 1:
            wait_sent(1, 0, send_a, sems_a)
        for core in range(2):
            wait_sent(half, core, send_b, sems_b)
    sent = update.at[:, 0:112, :]
    pltpu.make_async_copy(sent, sent, sems_c.at[0]).wait()
    pltpu.make_async_copy(out, out, sems_c.at[1]).wait()


VM = pl.BlockSpec(memory_space=pltpu.VMEM)
SM = pl.BlockSpec(memory_space=pltpu.SMEM)
ANY = pl.BlockSpec(memory_space=pl.ANY)


def on_device(
    spectral,
    legendre,
    wave_ids,
    trunc_lengths,
    cycle_points,
    grid_coef,
    cycle_weights,
    modes_in,
    modes_out,
    depths,
):
    pack, unpack, spread, back, packt, eye = [jnp.asarray(x, BF) for x in constant_arrays()]
    vmem = pltpu.VMEM
    return pl.pallas_call(
        whole,
        out_shape=pltpu.VMEM((4, 6, 16, NT), BF),
        in_specs=[ANY] * 17,
        out_specs=VM,
        scratch_shapes=[
            pltpu.SMEM((128,), jnp.int32),
            pltpu.SMEM((128,), jnp.int32),
            pltpu.SMEM((NT,), jnp.int32),
            vmem((1, 128), jnp.int32),
            vmem((1, 128), F32),
            vmem((128, 128), BF),
            vmem((128, 128), BF),
            vmem((128, NT), F32),
            vmem((384, NT), BF),
            vmem((4, 640, NT), BF),
            vmem((256, 240), BF),
            vmem((40, 2560), F32),
            vmem((256, 256), BF),
            vmem((96, 384), BF),
            vmem((256, 256), BF),
            vmem((240, 256), BF),
            vmem((256, 256), BF),
            vmem((6, 256, NT), BF),
            vmem((3, 640, 256), BF),
            vmem((2 * HALF, 128), BF),
            vmem((2 * HALF, 128), BF),
            vmem((4, 256, 256), BF),
            vmem((CYC, 256, 2560), BF),
            vmem((2, 128, 256), F32),
            vmem((CYC, 384, 256), BF),
            vmem((384, 2560), BF),
            vmem((CYC, 256, 384), BF),
            vmem((2 * HALF, 128), BF),
            vmem((2 * HALF, 128), BF),
            vmem((3, 640, 256), BF),
            vmem((768, 640), BF),
            vmem((3, 128, NT), BF),
            vmem((128, 128), F32),
            vmem((8, 128), F32),
            vmem((640, 128), F32),
            vmem((128, 128), F32),
            vmem((8, 128), F32),
            vmem((2, 8, 128), BF),
            vmem((2, 8, 128), BF),
            pltpu.SemaphoreType.DMA((7,)),
            pltpu.SemaphoreType.DMA((N_LATE,)),
            pltpu.SemaphoreType.REGULAR,
            pltpu.SemaphoreType.DMA((2, 4)),
            pltpu.SemaphoreType.DMA((2, 4)),
            pltpu.SemaphoreType.DMA((2,)),
        ],
        name="whole",
        compiler_params=pltpu.CompilerParams(
            vmem_limit_bytes=56 * 1024 * 1024, collective_id=0, has_side_effects=True
        ),
    )(
        trunc_lengths,
        wave_ids,
        cycle_points,
        spectral.reshape(384, NT),
        legendre,
        pack,
        grid_coef,
        unpack,
        spread,
        back,
        packt,
        eye,
        cycle_weights,
        wave_ids.reshape(1, 128),
        depths.reshape(1, 128),
        modes_in,
        modes_out,
    )


def solution(mesh):
    placed = (
        P("wave", None, "lev", None),
        P("wave", None, None),
        P(),
        P(),
        P(),
        P("wave", None),
        P(),
        P(),
        P(),
        P(),
    )
    return jax.shard_map(
        on_device,
        mesh=mesh,
        in_specs=placed,
        out_specs=P("wave", None, "lev", None),
        check_vma=False,
    )
```

```python
import jax
import jax.numpy as jnp
import numpy as np
from jax import lax
from jax.experimental import pallas as pl
from jax.experimental.pallas import tpu as pltpu
from jax.sharding import PartitionSpec as P

MESH = pl.DeviceIdType.MESH
NT = 1280
BF = jnp.bfloat16
F32 = jnp.float32
WAVES = 32
LEVS = 8
DEVS = 256
CYC = 5
UNROLL = 4
CHUNKS = ((0, 256), (256, 256), (512, 256), (768, 256), (1024, 256))
HALF = DEVS * 8
SECTIONS = ((0, 0, 0, 96), (0, 1, 96, 128), (1, 1, 0, 64), (1, 2, 64, 128), (2, 2, 0, 32), (2, 3, 32, 128))


def nt_dot(a, b):
    return lax.dot_general(a, b, (((1,), (1,)), ((), ())), preferred_element_type=F32)


def nn_dot(a, b):
    return lax.dot_general(a, b, (((1,), (0,)), ((), ())), preferred_element_type=F32)


def constant_arrays():
    half, rest = np.divmod(np.arange(256), 128)
    block, row = np.divmod(rest, 8)
    row = row + half * 8
    tile, cyc = np.divmod(np.arange(240), 80)
    pack = (row[:, None] < 15) & (row[:, None] % 3 == tile[None]) & (5 * block[:, None] + row[:, None] // 3 == cyc[None])
    out_row, out_w = np.divmod(np.arange(256), 32)
    in_w, in_row = np.divmod(np.arange(256), 8)
    unpack = (out_w[:, None] == in_w[None]) & (out_row[:, None] == in_row[None])
    spread = np.arange(96)[:, None] == np.arange(384)[None] % 96
    return [x.astype(np.float32) for x in (pack, unpack, spread, unpack.T, pack.T, np.eye(256))]


def position():
    return lax.axis_index("wave"), lax.axis_index("lev")


def shifted(dz, dy, dx, dc):
    w, s = position()
    tw = lax.rem(w // 4 + dz, 8) * 4 + lax.rem(w + dy, 4)
    return tw, lax.rem(s // 2 + dx, 4) * 2 + lax.rem(s + dc, 2)


def mirrored(dest):
    return jnp.where(dest < 128, dest, 383 - dest)


def inverse_rows(spec_ref, len_of, rhs):
    column = lax.broadcasted_iota(jnp.int32, (1, NT), 1)
    for idx, (t, m, lo, hi) in enumerate(SECTIONS):
        live = column < len_of(m)
        north = jnp.where(live, 1.0, 0.0).astype(BF)
        south = jnp.where(live, jnp.where(column % 2 == 0, 1.0, -1.0), 0.0).astype(BF)
        for half, factor in ((0, north), (128, south)):
            if lo > 0:
                rhs[idx, half : half + lo, :] = jnp.zeros((lo, NT), BF)
            if hi < 128:
                rhs[idx, half + hi : half + 128, :] = jnp.zeros((128 - hi, NT), BF)
            rhs[idx, half + lo : half + hi, :] = spec_ref[t * 128 + lo : t * 128 + hi, :] * factor


def inverse_dots(t, leg, rhs, waves_out):
    step = 320
    ma, mb = SECTIONS[2 * t][1], SECTIONS[2 * t + 1][1]

    def block(jc, _):
        rows = pl.ds(pl.multiple_of(jc * step, 64), step)
        out = nt_dot(leg[ma, rows, :], rhs[2 * t]) + nt_dot(leg[mb, rows, :], rhs[2 * t + 1])
        waves_out[t, rows, :] = out.astype(BF)
        return 0

    lax.fori_loop(0, 640 // step, block, 0, unroll=True)


def inverse_pack(pack, waves_out, send):
    def block(g, _):
        rows = pl.ds(pl.multiple_of(g * 80, 16), 80)
        x = jnp.concatenate([waves_out[t, rows, :] for t in range(3)], axis=0)
        y = nn_dot(pack[...], x).astype(BF)
        for half in range(2):
            for side in range(2):
                rows = pl.ds(pl.multiple_of(half * HALF + side * 1024 + g * 128, 128), 128)
                send[rows, :] = y[half * 128 : half * 128 + 128, side * 128 : side * 128 + 128]
        return 0

    lax.fori_loop(0, 8, block, 0, unroll=8)


def cos_sin(steps, count):
    turns = jnp.round(steps * (4.0 / count))
    rest = steps - turns * (count * 0.25)
    x = rest * (2.0 * np.pi / count)
    x2 = x * x
    sine = x * (1.0 + x2 * (-1.0 / 6 + x2 * (1.0 / 120 + x2 * (-1.0 / 5040 + x2 * (1.0 / 362880)))))
    cosine = 1.0 + x2 * (-0.5 + x2 * (1.0 / 24 + x2 * (-1.0 / 720 + x2 * (1.0 / 40320))))
    quadrant = turns.astype(jnp.int32) & 3
    swap = (quadrant & 1) == 1
    c = jnp.where(swap, sine, cosine)
    s = jnp.where(swap, cosine, sine)
    c = jnp.where((quadrant == 1) | (quadrant == 2), -c, c)
    s = jnp.where(quadrant >= 2, -s, s)
    return c, s


def cycle_table(u, wave_col, points, table, low):
    count = jnp.full((1, 128), points, jnp.int32).astype(F32)
    lane = lax.broadcasted_iota(jnp.int32, (1, 128), 1)
    lane_f = lane.astype(F32)
    waves = wave_col[...]
    for half in range(2):
        c, s = cos_sin(waves * (lane_f + 128.0 * half), count)
        low[0, :, half * 128 : half * 128 + 128] = c
        low[1, :, half * 128 : half * 128 + 128] = s
    c_high, s_high = cos_sin(waves * (lane_f * 256.0), count)
    live = 2.0 * waves < count
    c_high = jnp.where(live, c_high, 0.0)
    s_high = jnp.where(live, s_high, 0.0)
    wide = lax.broadcasted_iota(jnp.int32, (1, 256), 1)
    for a in range(10):
        ca = c_high[:, a : a + 1]
        sa = s_high[:, a : a + 1]
        keep = jnp.where(wide + 256 * a < points, 1.0, 0.0)
        cl = low[0] * keep
        sl = low[1] * keep
        cols = slice(a * 256, a * 256 + 256)
        table[u, 0:128, cols] = (cl * ca - sl * sa).astype(BF)
        table[u, 128:256, cols] = (-(sl * ca + cl * sa)).astype(BF)


def gather_waves(cycles, recv, unpack, spread, wave_row, split, fields):
    lane = lax.broadcasted_iota(jnp.int32, (1, 384), 1)
    sections = [jnp.where((lane >= 96 * m) & (lane < 96 * m + 96), 1.0, 0.0).astype(BF) for m in range(4)]
    factor = jnp.where(wave_row[0:1, :] == 0.0, 1.0, 2.0)

    def pair(sp, _):
        def sorted_half(half):
            starts = [pl.multiple_of(half * HALF + sp * 512 + h * 256, 256) for h in range(2)]
            return nn_dot(unpack[...], jnp.concatenate([recv[pl.ds(x, 256), :] for x in starts], axis=1)).astype(BF)

        if cycles == (0, 1):
            z = sorted_half(0)
            split[sp, 0:64] = z[192:256]
            rows_of = {u: [z[96 * u + 32 * t : 96 * u + 32 * t + 32] for t in range(3)] for u in cycles}
        elif cycles == (2,):
            z = sorted_half(1)
            split[sp, 64:256] = z[32:224]
            rows_of = {2: [split[sp, 0:32], split[sp, 32:64], z[0:32]]}
        else:
            rows_of = {u: [split[sp, 96 * u - 224 + 32 * t : 96 * u - 192 + 32 * t] for t in range(3)] for u in cycles}
        for u, tiles in rows_of.items():
            pieces = []
            for h in range(2):
                zu = jnp.concatenate([x[:, h * 128 : h * 128 + 128] for x in tiles], axis=1)
                pieces += [zu * sections[m] for m in range(4)]
            y = nt_dot(spread[...], jnp.concatenate(pieces, axis=0))
            for h in range(2):
                part = (y[:, h * 128 : h * 128 + 128] * factor).astype(BF)
                for r in range(2):
                    for f in range(3):
                        rows = pl.ds(pl.multiple_of(f * 128 + sp * 32 + h * 16, 16), 16)
                        fields[u, rows, r * 128 : r * 128 + 128] = part[r * 48 + f * 16 : r * 48 + f * 16 + 16, :]
        return 0

    lax.fori_loop(0, 4, pair, 0, unroll=4)


def grid_cycle(u, points, coef_row, table, fields, tend, analysed):
    for a in range(10):
        cols = slice(a * 256, a * 256 + 256)
        g = nn_dot(fields[u], table[u, :, cols])
        coef = coef_row[:, cols]
        for f in range(3):
            nxt = (f + 1) % 3
            tend[f * 128 : f * 128 + 128, cols] = (
                g[f * 128 : f * 128 + 128] * (coef + g[nxt * 128 : nxt * 128 + 128])
            ).astype(BF)
    total = nt_dot(table[u], tend[...])
    share = 1.0 / jnp.full((1, 384), points, jnp.int32).astype(F32)
    analysed[u] = (total * share).astype(BF)


def pack_return(half, back, analysed, send):
    places = [divmod(half * 8 + i, 3) for i in range(8)]

    def pair(g, _):
        groups = []
        for h in range(2):
            rows = pl.ds(pl.multiple_of(g * 64 + h * 32, 32), 32)
            groups.append(
                jnp.concatenate(
                    [
                        analysed[u, rows, f * 128 : f * 128 + 128] if u < CYC else jnp.zeros((32, 128), BF)
                        for u, f in places
                    ],
                    axis=0,
                )
            )
        y = nn_dot(back[...], jnp.concatenate(groups, axis=1)).astype(BF)
        for h in range(2):
            rows = pl.ds(pl.multiple_of(half * HALF + g * 512 + h * 256, 256), 256)
            send[rows, :] = y[:, h * 128 : h * 128 + 128]
        return 0

    lax.fori_loop(0, 4, pair, 0, unroll=4)


def parity_parts(recv, packt, weight_col, parts):
    def block(g, _):
        rows = pl.ds(pl.multiple_of(g * 80, 16), 80)
        sides = []
        for side in range(2):
            starts = [pl.multiple_of(half * HALF + side * 1024 + g * 128, 128) for half in range(2)]
            sides.append(jnp.concatenate([recv[pl.ds(x, 128), :] for x in starts], axis=0))
        x = jnp.concatenate(sides, axis=1)
        z = nn_dot(packt[...], x)
        weight = weight_col[rows, :]
        for f in range(3):
            north = z[f * 80 : f * 80 + 80, :128]
            south = z[f * 80 : f * 80 + 80, 128:]
            parts[f, rows, 0:128] = (weight * (north + south)).astype(BF)
            parts[f, rows, 128:256] = (weight * (north - south)).astype(BF)
        return 0

    lax.fori_loop(0, 8, block, 0, unroll=8)


def make_damp(wave, depth_col, damp):
    for a in range(NT // 128):
        degree = (lax.broadcasted_iota(jnp.int32, (1, 128), 1) + (wave + a * 128)).astype(F32)
        damp[:, a * 128 : a * 128 + 128] = 1.0 / (1.0 + depth_col[...] * degree * (degree + 1.0) / float(NT * NT))


def forward_modes(leg_m, length, eye, parts, flipped, modes_in, modes_out, damp, update, ready):
    for f in range(3):
        t = nt_dot(eye[...], parts[f]).astype(BF)
        flipped[f * 128 : f * 128 + 128, :] = t[:128]
        flipped[384 + f * 128 : 512 + f * 128, :] = t[128:]
    lane = lax.broadcasted_iota(jnp.int32, (1, 256), 1)
    even_lane = lane % 2 == 0

    def project(start, width):
        both = nn_dot(flipped[...], leg_m(slice(start, start + width)))
        live = lane[:, :width] + start < length
        parts = []
        for f in range(3):
            even = both[f * 128 : f * 128 + 128]
            odd = both[384 + f * 128 : 512 + f * 128]
            parts.append(jnp.where(live, jnp.where(even_lane[:, :width], even, odd), 0.0).astype(BF))
        return jnp.concatenate(parts, axis=1)

    def mix(start, width, proj):
        cols = slice(start, start + width)
        vals = nn_dot(modes_in[...], proj)
        scaled = (vals * jnp.concatenate([damp[:, cols]] * 3, axis=1)).astype(BF)
        mixed = nn_dot(modes_out[...], scaled).astype(BF)
        for f in range(3):
            update[f, :, cols] = mixed[:, f * width : f * width + width]

    proj = project(*CHUNKS[0])
    for chunk, following in zip(CHUNKS, CHUNKS[1:] + (None,)):
        after = project(*following) if following else None
        mix(*chunk, proj)
        ready(*chunk)
        proj = after


def column_of(row):
    return jnp.transpose(jnp.broadcast_to(row, (128, 128)))


def side_columns(waves_row, weights, depths_row, wave_col, wave_row, weight_col, depth_col):
    place = lax.broadcasted_iota(jnp.int32, (128, 128), 0)
    slot = lax.broadcasted_iota(jnp.int32, (128, 128), 1)
    order = jnp.where((place % 32) * 4 + place // 32 == slot, 1.0, 0.0).astype(BF)
    rows = jnp.broadcast_to(waves_row[...], (128, 128))
    high = (rows // 32).astype(F32).astype(BF)
    low = (rows % 32).astype(F32).astype(BF)
    column = nt_dot(order, high) * 32.0 + nt_dot(order, low)
    wave_col[...] = column
    wave_row[...] = jnp.transpose(column)[0:8]
    for i in range(5):
        weight_col[i * 128 : i * 128 + 128, :] = column_of(weights[i : i + 1, :])
    depth_col[...] = column_of(depths_row[...])


def send_class(half, core, send, recv, spare, sems, source_slot, my_slot):
    w, s = position()

    def rows(slot):
        return pl.ds(pl.multiple_of(half * HALF + slot * 8, 8), 8)

    def start(tw, ts):
        pltpu.make_async_remote_copy(
            src_ref=send.at[rows(source_slot(tw, ts))],
            dst_ref=recv.at[rows(my_slot)],
            send_sem=sems.at[half, core],
            recv_sem=sems.at[half, 2],
            device_id=(tw, ts),
            device_id_type=MESH,
        ).start()

    for k in range(LEVS // 2):
        ts = ((s // 2 + k) & 3) * 2 + core
        if k == 0:
            own = (s & 1) == core
            pl.when(jnp.logical_not(own))(lambda ts=ts: start(w, ts))

            @pl.when(own)
            def _():
                source = send.at[rows(source_slot(w, s))]
                pltpu.make_async_copy(source, recv.at[rows(my_slot)], sems.at[half, 3]).start()
                pltpu.make_async_copy(source, spare.at[half], sems.at[half, core]).start()

        else:
            start(w, ts)
        lax.fori_loop(1, WAVES, lambda i, c, ts=ts: (start((w + i) & 31, ts), c)[1], 0, unroll=UNROLL)


def wait_sent(half, core, send, sems):
    part = send.at[pl.ds(half * HALF, HALF // 2)]
    pltpu.make_async_copy(part, part, sems.at[half, core]).wait()


def wait_half(half, recv, sems):
    rest = recv.at[pl.ds(half * HALF, HALF - 8)]
    own = recv.at[pl.ds(half * HALF, 8)]
    pltpu.make_async_copy(own, own, sems.at[half, 3]).wait()
    pltpu.make_async_copy(rest, rest, sems.at[half, 2]).wait()


def signal_peers(sem, peers):
    for peer in peers:
        pl.semaphore_signal(sem, inc=1, device_id=shifted(*peer), device_id_type=MESH)


PLANE_PEERS = [(0, dy, dx, dc) for dx in range(4) for dy in range(4) for dc in range(2) if dx or dy or dc]
Z_PEERS = [(dz, 0, 0, 0) for dz in range(1, 8)]
N_LATE = 17


def whole(
    lens_hbm,
    waves_hbm,
    cyc_hbm,
    spec_hbm,
    leg_hbm,
    pack_hbm,
    coef_hbm,
    unpack_hbm,
    spread_hbm,
    back_hbm,
    packt_hbm,
    eye_hbm,
    weights_hbm,
    waves_row_hbm,
    depths_row_hbm,
    modes_in_hbm,
    modes_out_hbm,
    out,
    lens,
    waves,
    cyc,
    waves_row,
    depths_row,
    modes_in,
    modes_out,
    damp,
    spec,
    leg,
    pack,
    coef,
    unpack,
    spread,
    back,
    packt,
    eye,
    rhs,
    waves_out,
    send_a,
    recv_a,
    split,
    table,
    low,
    fields,
    tend,
    analysed,
    send_b,
    recv_b,
    parts,
    flipped,
    update,
    wave_col,
    wave_row,
    weight_col,
    depth_col,
    weights,
    spare_a,
    spare_b,
    load_sem,
    late_sem,
    z_sem,
    sems_a,
    sems_b,
    sems_c,
):
    w, s = position()
    dest = w * LEVS + s
    m, r = s // 2, lax.rem(s, 2)
    barrier = pltpu.get_barrier_semaphore()

    loads = [pltpu.make_async_copy(spec_hbm, spec, load_sem.at[0])]
    loads += [pltpu.make_async_copy(leg_hbm.at[i], leg.at[i], load_sem.at[1 + i]) for i in range(4)]
    loads += [pltpu.make_async_copy(pack_hbm, pack, load_sem.at[5]), pltpu.make_async_copy(lens_hbm, lens, load_sem.at[6])]
    late = [
        pltpu.make_async_copy(a, b, late_sem.at[i])
        for i, (a, b) in enumerate(
            [
                (coef_hbm, coef),
                (unpack_hbm, unpack),
                (spread_hbm, spread),
                (back_hbm, back),
                (packt_hbm, packt),
                (eye_hbm, eye),
                (waves_hbm, waves),
                (cyc_hbm, cyc),
                (waves_row_hbm, waves_row),
                (depths_row_hbm, depths_row),
                (modes_in_hbm, modes_in),
                (modes_out_hbm, modes_out),
                *[(weights_hbm.at[pl.ds(i * 128, 128)], weights.at[i]) for i in range(5)],
            ]
        )
    ]
    for copy in [loads[6]] + loads[:6] + late:
        copy.start()

    signal_peers(barrier, Z_PEERS + PLANE_PEERS)
    loads[6].wait()
    loads[0].wait()
    inverse_rows(spec, lambda i: lens[w * 4 + i], rhs)
    loads[1].wait()
    loads[2].wait()
    inverse_dots(0, leg, rhs, waves_out)
    pl.semaphore_wait(barrier, len(Z_PEERS + PLANE_PEERS))
    signal_peers(z_sem, Z_PEERS)
    loads[3].wait()
    inverse_dots(1, leg, rhs, waves_out)
    loads[4].wait()
    inverse_dots(2, leg, rhs, waves_out)
    loads[5].wait()
    inverse_pack(pack, waves_out, send_a)
    pl.semaphore_wait(z_sem, len(Z_PEERS))

    def to_cycles(half, core):
        send_class(half, core, send_a, recv_a, spare_a, sems_a, lambda tw, ts: mirrored(tw * LEVS + ts), s * WAVES + w)

    def to_waves(half, core):
        send_class(
            half,
            core,
            send_b,
            recv_b,
            spare_b,
            sems_b,
            lambda tw, ts: ((ts & 1) * 4 + (ts >> 1)) * 32 + tw,
            mirrored(w * LEVS + s),
        )

    def shift(u):
        return jnp.where(dest < 128, u, 4 - u)

    def make_table(u, _):
        cycle_table(u, wave_col, cyc[dest * CYC + shift(u)], table, low)
        return 0

    to_cycles(0, 0)
    for copy in late:
        copy.wait()
    side_columns(waves_row, weights, depths_row, wave_col, wave_row, weight_col, depth_col)
    make_table(0, 0)
    to_cycles(1, 0)
    lax.fori_loop(1, CYC, make_table, 0)
    wait_sent(0, 0, send_a, sems_a)
    to_cycles(0, 1)
    to_cycles(1, 1)

    def cycle(u, _):
        points = cyc[dest * CYC + shift(u)]
        grid_cycle(u, points, coef[pl.ds(s * CYC + shift(u), 1), :], table, fields, tend, analysed)
        return 0

    wait_half(0, recv_a, sems_a)
    gather_waves((0, 1), recv_a, unpack, spread, wave_row, split, fields)
    lax.fori_loop(0, 2, cycle, 0)
    wait_half(1, recv_a, sems_a)
    gather_waves((2,), recv_a, unpack, spread, wave_row, split, fields)
    cycle(2, 0)
    pack_return(0, back, analysed, send_b)
    to_waves(0, 0)
    gather_waves((3, 4), recv_a, unpack, spread, wave_row, split, fields)
    pl.when((s & 1) == 0)(lambda: to_waves(0, 1))
    lax.fori_loop(3, CYC, cycle, 0)
    pack_return(1, back, analysed, send_b)
    to_waves(1, 0)
    pl.when((s & 1) == 1)(lambda: to_waves(0, 1))
    make_damp(waves[w * 4 + m], depth_col, damp)
    to_waves(1, 1)
    for half in range(2):
        wait_half(half, recv_b, sems_b)

    def to_levels(start, width):
        cols = pl.ds(start, width)
        place = out.at[m, pl.ds(r * 3, 3), :, cols]

        def piece(ts):
            return update.at[:, pl.ds(pl.multiple_of(ts * 16, 16), 16), cols]

        for i in range(1, LEVS):
            ts = lax.rem(s + i, LEVS)
            pltpu.make_async_remote_copy(
                src_ref=piece(ts),
                dst_ref=place,
                send_sem=sems_c.at[0],
                recv_sem=sems_c.at[1],
                device_id=(w, ts),
                device_id_type=MESH,
            ).start()
        pltpu.make_async_copy(piece(s), place, sems_c.at[1]).start()

    parity_parts(recv_b, packt, weight_col, parts)
    forward_modes(
        lambda cols: leg[m, :, cols],
        lens[w * 4 + m],
        eye,
        parts,
        flipped,
        modes_in,
        modes_out,
        damp,
        update,
        to_levels,
    )
    for half in range(2):
        wait_sent(half, 1, send_a, sems_a)
        if half == 1:
            wait_sent(1, 0, send_a, sems_a)
        for core in range(2):
            wait_sent(half, core, send_b, sems_b)
    sent = update.at[:, 0:112, :]
    pltpu.make_async_copy(sent, sent, sems_c.at[0]).wait()
    pltpu.make_async_copy(out, out, sems_c.at[1]).wait()


VM = pl.BlockSpec(memory_space=pltpu.VMEM)
SM = pl.BlockSpec(memory_space=pltpu.SMEM)
ANY = pl.BlockSpec(memory_space=pl.ANY)


def on_device(
    spectral,
    legendre,
    wave_ids,
    trunc_lengths,
    cycle_points,
    grid_coef,
    cycle_weights,
    modes_in,
    modes_out,
    depths,
):
    pack, unpack, spread, back, packt, eye = [jnp.asarray(x, BF) for x in constant_arrays()]
    vmem = pltpu.VMEM
    return pl.pallas_call(
        whole,
        out_shape=pltpu.VMEM((4, 6, 16, NT), BF),
        in_specs=[ANY] * 17,
        out_specs=VM,
        scratch_shapes=[
            pltpu.SMEM((128,), jnp.int32),
            pltpu.SMEM((128,), jnp.int32),
            pltpu.SMEM((NT,), jnp.int32),
            vmem((1, 128), jnp.int32),
            vmem((1, 128), F32),
            vmem((128, 128), BF),
            vmem((128, 128), BF),
            vmem((128, NT), F32),
            vmem((384, NT), BF),
            vmem((4, 640, NT), BF),
            vmem((256, 240), BF),
            vmem((40, 2560), F32),
            vmem((256, 256), BF),
            vmem((96, 384), BF),
            vmem((256, 256), BF),
            vmem((240, 256), BF),
            vmem((256, 256), BF),
            vmem((6, 256, NT), BF),
            vmem((3, 640, 256), BF),
            vmem((2 * HALF, 128), BF),
            vmem((2 * HALF, 128), BF),
            vmem((4, 256, 256), BF),
            vmem((CYC, 256, 2560), BF),
            vmem((2, 128, 256), F32),
            vmem((CYC, 384, 256), BF),
            vmem((384, 2560), BF),
            vmem((CYC, 256, 384), BF),
            vmem((2 * HALF, 128), BF),
            vmem((2 * HALF, 128), BF),
            vmem((3, 640, 256), BF),
            vmem((768, 640), BF),
            vmem((3, 128, NT), BF),
            vmem((128, 128), F32),
            vmem((8, 128), F32),
            vmem((640, 128), F32),
            vmem((128, 128), F32),
            vmem((8, 128), F32),
            vmem((2, 8, 128), BF),
            vmem((2, 8, 128), BF),
            pltpu.SemaphoreType.DMA((7,)),
            pltpu.SemaphoreType.DMA((N_LATE,)),
            pltpu.SemaphoreType.REGULAR,
            pltpu.SemaphoreType.DMA((2, 4)),
            pltpu.SemaphoreType.DMA((2, 4)),
            pltpu.SemaphoreType.DMA((2,)),
        ],
        name="whole",
        compiler_params=pltpu.CompilerParams(
            vmem_limit_bytes=56 * 1024 * 1024, collective_id=0, has_side_effects=True
        ),
    )(
        trunc_lengths,
        wave_ids,
        cycle_points,
        spectral.reshape(384, NT),
        legendre,
        pack,
        grid_coef,
        unpack,
        spread,
        back,
        packt,
        eye,
        cycle_weights,
        wave_ids.reshape(1, 128),
        depths.reshape(1, 128),
        modes_in,
        modes_out,
    )


def solution(mesh):
    placed = (
        P("wave", None, "lev", None),
        P("wave", None, None),
        P(),
        P(),
        P(),
        P("wave", None),
        P(),
        P(),
        P(),
        P(),
    )
    return jax.shard_map(
        on_device,
        mesh=mesh,
        in_specs=placed,
        out_specs=P("wave", None, "lev", None),
        check_vma=False,
    )
```
